32 devices in a mesh: gx: 4 (over x, core), gy: 2 (over y), gz: 4 (over z).
Axes of the slice: x: 2, y: 2, z: 4, core: 2. Of those that a mesh axis runs over, the one named last changes fastest.
Arguments:
- positions: float32 [3, 4, 2, 4, 256], P(None, 'gx', 'gy', 'gz'), may hold values from 0 to 4, as said below
- velocities: float32 [3, 4, 2, 4, 256], P(None, 'gx', 'gy', 'gz'), may hold values from -6 to 6
- forces: float32 [3, 4, 2, 4, 256], P(None, 'gx', 'gy', 'gz'), may hold values from -6 to 6
- charges: float32 [4, 2, 4, 256], P('gx', 'gy', 'gz'), may hold values from -2 to 2
- inverse_mass: float32 [4, 2, 4, 256], P('gx', 'gy', 'gz'), may hold values from 0.5 to 2
- occupancy: int32 [4, 2, 4], P('gx', 'gy', 'gz'), may hold values from 128 to 256
- molecule: int32 [4, 2, 4, 256], P('gx', 'gy', 'gz'), may hold values from 0 to 127, never falling along the last dimension, each value on 1 to 4 neighbouring positions
Outputs:
- positions_out: float32 [3, 4, 2, 4, 256], P(None, 'gx', 'gy', 'gz')
- velocities_out: float32 [3, 4, 2, 4, 256], P(None, 'gx', 'gy', 'gz')
- forces_out: float32 [3, 4, 2, 4, 256], P(None, 'gx', 'gy', 'gz')
The draws below stay inside these ranges and needn't reach their ends.
Inputs may be any that keep to these rules, and one draw needn't show every extreme that they name: `positions`: component c of a particle of the box with index k along dimension c lies in [k, k + 1).
All inputs are finite; a program needn't handle non-finite values.
Results may differ from the reference program's by a relative error of at most 0.0003.
Values sent between devices are 32-bit elements; how exact they have to be, the bound alone decides.
No kernel may reach another device: no remote copies, remote signals or barrier semaphores. Data moves between devices by JAX's collectives and lax.ppermute only.
A program may use at most 64 MiB of HBM per device.

```python
import math
import jax
import jax.numpy as jnp
import numpy as np
from jax import lax

P_SIZE = 256
NX = 4
NY = 2
NZ = 4


def draw_positions(key, part):
    shape = (3, NX, NY, NZ, P_SIZE)
    inside = jax.random.uniform(key, shape, dtype=jnp.float32)
    first = jnp.arange(NX, dtype=jnp.float32)[:, None, None, None]
    second = jnp.arange(NY, dtype=jnp.float32)[None, :, None, None]
    third = jnp.arange(NZ, dtype=jnp.float32)[None, None, :, None]
    zeros = jnp.zeros((NX, NY, NZ, P_SIZE), dtype=jnp.float32)
    corner = jnp.stack([first + zeros, second + zeros, third + zeros])
    return (corner + inside).astype(jnp.float32)


def plant(drawn, key, smallest, largest):
    extent = drawn.shape
    index_at = [jax.random.randint(jax.random.fold_in(key, axis), (), 0, extent[axis]) for axis in range(len(extent))]
    drawn = drawn.at[tuple(index_at)].set(smallest)
    longest = extent.index(max(extent))
    index_at[longest] = (index_at[longest] + 1) % extent[longest]
    return drawn.at[tuple(index_at)].set(largest)


def levels(key, dims, pieces, least, top_value):
    level = 1.0
    for axis_at, shards_of in pieces:
        steps = jax.random.uniform(jax.random.fold_in(jax.random.fold_in(key, 6), axis_at), (shards_of,), jnp.float32, least / len(pieces), top_value / len(pieces))
        level = level * jnp.repeat(jnp.exp(steps), dims[axis_at] // shards_of).reshape((-1,) + (1,) * (len(dims) - 1 - axis_at))
    return level


def length_profile(number_of, total, most, lean):
    weights = [(1 << 20) // math.isqrt(standing ** lean) + 1 for standing in range(2, number_of + 1)]
    spare, counts = total - most - (number_of - 1), [1] * (number_of - 1)
    while spare > 0:
        free = [i for i in range(number_of - 1) if counts[i] < most]
        mass, remaining = sum([weights[i] for i in free]), spare
        for i in free:
            more = min(most - counts[i], max(1, remaining * weights[i] // mass), spare)
            counts[i] = counts[i] + more
            spare = spare - more
    return np.array([most] + counts)


def ragged_sizes(rng, amount, total, most, lean):
    if amount == 2:
        one = jax.random.randint(rng, (), max(1, total - most), min(most, total - 1) + 1)
        return jnp.stack([one, total - one])
    tallies = jnp.asarray(length_profile(amount, total, most, lean), jnp.int32)
    pairs = (amount - 1) // 2
    source_of, receiver = tallies[1:1 + 2 * pairs:2], tallies[2:2 + 2 * pairs:2]
    slack = jnp.minimum(source_of - 1, most - receiver)
    shifted = jax.random.randint(jax.random.fold_in(rng, 1), (pairs,), 0, 1 << 20) % (slack + 1)
    tallies = tallies.at[1:1 + 2 * pairs:2].set(source_of - shifted).at[2:2 + 2 * pairs:2].set(receiver + shifted)
    return tallies[jax.random.permutation(jax.random.fold_in(rng, 2), amount)]


def bell_draw(stream_key, shape, spread, most, shards=(), held_as=jnp.bfloat16):
    result = jax.random.normal(stream_key, shape, jnp.float32) * spread
    if len(shards) > 0:
        result = levels(stream_key, shape, shards, -0.22, 0.18) * result
    return jnp.clip(result, min=-most, max=most).astype(held_as)


def setup_inputs(seed: int = 0) -> dict:
    key_list = jax.random.split(jax.random.key(seed), 8)
    positions = draw_positions(jax.random.fold_in(key_list[7], 71), 0)
    velocities = bell_draw(key_list[1], (3, NX, NY, NZ, P_SIZE), 1.0, 6.0, ((1, 4), (2, 2), (3, 4)), jnp.float32)
    forces = bell_draw(key_list[2], (3, NX, NY, NZ, P_SIZE), 1.0, 6.0, ((1, 4), (2, 2), (3, 4)), jnp.float32)
    charges = bell_draw(key_list[3], (NX, NY, NZ, P_SIZE), 0.15, 2.0, ((0, 4), (1, 2), (2, 4)), jnp.float32)
    inverse_mass = jnp.clip(jnp.exp(math.log(2.0) - 1.3862944 * jax.random.uniform(key_list[4], (NX, NY, NZ, P_SIZE), jnp.float32) ** levels(key_list[4], (NX, NY, NZ, P_SIZE), ((0, 4), (1, 2), (2, 4)), -0.2, 0.2)), 0.5, 2.0)
    occupancy = plant(jax.random.randint(key_list[5], (NX, NY, NZ), P_SIZE // 2, P_SIZE + 1), jax.random.fold_in(key_list[5], 1), P_SIZE // 2, P_SIZE).astype(jnp.int32)
    molecule = jax.vmap(lambda own: jnp.searchsorted(jnp.cumsum(ragged_sizes(own, P_SIZE // 2, P_SIZE, 4, 0)), jnp.arange(P_SIZE), side="right"))(jax.random.split(key_list[6], NX * NY * NZ)).reshape((NX, NY, NZ, P_SIZE)).astype(jnp.int32)
    return dict(positions=positions, velocities=velocities, forces=forces, charges=charges, inverse_mass=inverse_mass, occupancy=occupancy, molecule=molecule)


cutoff_square = 4.0
soften_square = 0.25
time_step = 0.1
half_step = 0.05

def interact(target_places, target_charge, source_places, source_charge, lengths, pair_mask):
    separations = []
    for component in range(3):
        spacing = target_places[component][..., :, None] - source_places[component][..., None, :]
        separations.append(spacing - lengths[component] * jnp.floor(spacing / lengths[component] + 0.5))
    squared = separations[0] * separations[0] + separations[1] * separations[1] + separations[2] * separations[2]
    switch = jnp.maximum(1.0 - squared / cutoff_square, 0.0)
    soften = squared + soften_square
    weight = source_charge[..., None, :] * switch * switch / (soften * jnp.sqrt(soften))
    if pair_mask is not None:
        weight = weight * pair_mask
    return jnp.stack([target_charge * lax.optimization_barrier(jnp.sum(weight * separation, axis=-1)) for separation in separations])

def reach_list(cycle_size):
    if cycle_size >= 5:
        return list(range(-2, 3))
    return list(range(cycle_size))

def reference(positions, velocities, forces, charges, inverse_mass, occupancy, molecule):
    lengths = (float(NX), float(NY), float(NZ))
    slots = jnp.arange(P_SIZE, dtype=jnp.int32)
    charge_live = jnp.where(slots < occupancy[..., None], charges, jnp.float32(0.0))
    same_molecule = (molecule[..., :, None] == molecule[..., None, :]).astype(jnp.float32)
    table = np.array([(first, second, third) for first in reach_list(NX) for second in reach_list(NY) for third in reach_list(NZ)], dtype=np.int32)
    offsets = jnp.asarray(table).astype(jnp.int32)

    def force_field(places):
        sources = jnp.concatenate([places, charge_live[None]], axis=0)

        def advance(summed, offset):
            moved = jnp.roll(sources, (-offset[0], -offset[1], -offset[2]), axis=(1, 2, 3))
            return (summed + interact(places, charge_live, moved[:3], moved[3], lengths, None), None)
        summed, unused = lax.scan(advance, jnp.zeros_like(places), offsets)
        return summed - interact(places, charge_live, places, charge_live, lengths, same_molecule)
    places, velocity, current = (positions, velocities, forces)
    for turn in range(2):
        midway = velocity + half_step * inverse_mass * current
        places = places + time_step * midway
        current = force_field(places)
        velocity = midway + half_step * inverse_mass * current
    return (places, velocity, current)
```

```python
import functools
import math

import jax
import jax.numpy as jnp
from jax import lax
from jax.experimental import pallas as pl
from jax.experimental.pallas import tpu as pltpu
from jax.sharding import PartitionSpec as P

cutoff_square = 4.0
soften_square = 0.25
time_step = 0.1
half_step = 0.05

LANES = 128
ROWS = 8
TOGETHER = 4
TIE_SHIFT = 160
FULL = 4294967296.0


class Sizes:
    def __init__(self, lengths):
        self.lengths = lengths
        self.unit = max(set(lengths), key=lengths.count)
        step = self.unit / FULL
        self.top = cutoff_square / step**2
        self.soft = soften_square / step**2
        self.ratio = [(length / self.unit) ** 2 for length in lengths]
        self.scale = [
            (1.0 / (cutoff_square * cutoff_square)) * step * (length / FULL) for length in lengths
        ]
        self.shift = [TIE_SHIFT if length * length / 4 < cutoff_square else 0 for length in lengths]


def row_constant(values):
    row = lax.broadcasted_iota(jnp.int32, (ROWS, LANES), 0) // 2
    out = jnp.zeros((ROWS, LANES), jnp.float32)
    for c, value in enumerate(values):
        out = jnp.where(row == c, jnp.float32(value), out)
    return out


def to_steps(values, inverse):
    turns = values * inverse
    turns = turns - jnp.round(turns)
    turns = jnp.where(turns >= 0.5, -0.5, turns)
    return (turns * jnp.float32(FULL)).astype(jnp.int32)


def pair_weight(target, source, charge, sizes):
    parts = [(t - s).astype(jnp.float32) for t, s in zip(target, source)]
    squared = None
    for part, ratio in sorted(zip(parts, sizes.ratio), key=lambda item: item[1] != 1.0):
        square = part * part
        if ratio != 1.0:
            square = square * jnp.float32(ratio)
        squared = square if squared is None else squared + square
    switch = jnp.maximum(jnp.float32(sizes.top) - squared, 0.0)
    root = lax.rsqrt(squared + jnp.float32(sizes.soft))
    first = switch * root
    return parts, (first * first) * (root * charge)


def start_kernel(pos, vel, frc, chg, imass, occ, send, own, mid, mass, charge):
    live = lax.broadcasted_iota(jnp.int32, (1, 2 * LANES), 1) < occ[0, 0, 0]
    live_charge = jnp.where(live, chg[0, 0], 0.0)
    inverse = imass[0, 0]
    for h in range(2):
        cut = slice(h * LANES, (h + 1) * LANES)
        for c in range(3):
            r = slice(2 * c + h, 2 * c + h + 1)
            midway = vel[c, 0, 0] + half_step * inverse * frc[c, 0, 0]
            places = pos[c, 0, 0] + time_step * midway
            own[r, :] = places[:, cut]
            mid[r, :] = midway[:, cut]
            mass[r, :] = inverse[:, cut]
            charge[r, :] = live_charge[:, cut]
        r = slice(6 + h, 7 + h)
        own[r, :] = live_charge[:, cut]
        mid[r, :] = jnp.zeros((1, LANES), jnp.float32)
        mass[r, :] = jnp.zeros((1, LANES), jnp.float32)
        charge[r, :] = jnp.zeros((1, LANES), jnp.float32)
    block = own[...]
    for b in range(send.shape[0]):
        send[b] = block


def pack_sources(boxes, packed, steps, inverse):
    count = boxes.shape[0]
    lane = lax.broadcasted_iota(jnp.int32, (ROWS, LANES), 1)
    row = lax.broadcasted_iota(jnp.int32, (ROWS, LANES), 0)
    odd = lax.rem(row, 2) == 1
    filled = []
    for b in range(count):
        tail = boxes[b, 7:8, :]
        filled.append(jnp.max(jnp.where(tail != 0.0, lane[:1] + 1, 0)))
    position = jnp.int32(0)
    packed[0] = jnp.zeros((ROWS, LANES), jnp.float32)
    for b in range(count):
        tile = position // LANES
        begin = lax.rem(position, LANES)
        moved = pltpu.roll(boxes[b], begin, 1)
        packed[tile] = jnp.where(lane >= begin, moved, packed[tile])
        packed[tile + 1] = jnp.where(lane < begin, moved, 0.0)
        position = position + filled[b]
    tiles = (position + (LANES - 1)) // LANES
    for b in range(count):
        both = jnp.where(odd, packed[b], boxes[b])
        packed[b] = both
        steps[b] = to_steps(both, inverse)
    return tiles


def force_of(boxes, own, charge, labels, packed, steps, targets, sums, sizes):
    count = boxes.shape[0]
    inverse = row_constant([1.0 / length for length in sizes.lengths])
    tiles = pack_sources(boxes, packed, steps, inverse)
    mine = to_steps(own[...], inverse)
    columns = jnp.transpose(mine)
    for c in range(3):
        for h in range(2):
            for g in range(16):
                column = columns[8 * g : 8 * g + 8, 2 * c + h : 2 * c + h + 1]
                targets[c, 16 * h + g] = jnp.broadcast_to(column, (ROWS, LANES)) + sizes.shift[c]

    def over_targets(turn, unused):
        first = turn * TOGETHER
        target = [[targets[c, first + j] for c in range(3)] for j in range(TOGETHER)]

        def over_sources(k, totals, halves):
            totals = list(totals)
            for h in halves:
                source = [
                    jnp.broadcast_to(steps[k, 2 * c + h : 2 * c + h + 1, :], (ROWS, LANES))
                    for c in range(3)
                ]
                weight = jnp.broadcast_to(packed[k, 6 + h : 7 + h, :], (ROWS, LANES))
                for j in range(TOGETHER):
                    parts, base = pair_weight(target[j], source, weight, sizes)
                    for c in range(3):
                        totals[3 * j + c] = totals[3 * j + c] + base * parts[c]
            return tuple(totals)

        totals = (jnp.zeros((ROWS, LANES), jnp.float32),) * (3 * TOGETHER)
        totals = lax.fori_loop(0, tiles, lambda k, t: over_sources(k, t, (0, 1)), totals)
        totals = lax.fori_loop(tiles, count, lambda k, t: over_sources(k, t, (0,)), totals)
        for j in range(TOGETHER):
            for c in range(3):
                sums[c, pl.ds(pl.multiple_of((first + j) * ROWS, ROWS), ROWS), :] = totals[3 * j + c]
        return unused

    lax.fori_loop(0, 32 // TOGETHER, over_targets, 0)

    def spread(array):
        line = jnp.concatenate([array[0:1, :], array[1:2, :]], axis=1)
        return jnp.broadcast_to(line, (ROWS, 2 * LANES))

    def shifted(array):
        return pltpu.roll(pltpu.roll(array, 2 * LANES - 3, 1), 0, 1, stride=1, stride_axis=0)

    here = [spread(mine[2 * c : 2 * c + 2]) for c in range(3)]
    there = [shifted(array) for array in here]
    charge_there = shifted(spread(charge[0:2, :]))
    label = jnp.broadcast_to(labels[0, 0], (ROWS, 2 * LANES))
    slot = lax.broadcasted_iota(jnp.int32, (ROWS, 2 * LANES), 1)
    away = lax.broadcasted_iota(jnp.int32, (ROWS, 2 * LANES), 0)
    other = slot + 3 - away
    same = (shifted(label) == label) & (other >= 0) & (other < 2 * LANES) & (away < 7)
    here = [array + shift for array, shift in zip(here, sizes.shift)]
    parts, base = pair_weight(here, there, jnp.where(same, charge_there, 0.0), sizes)

    row = lax.broadcasted_iota(jnp.int32, (ROWS, LANES), 0)
    ones = jnp.ones((ROWS, LANES), jnp.float32)
    result = jnp.zeros((ROWS, LANES), jnp.float32)
    for c in range(3):
        every = lax.dot_general(
            ones, sums[c], (((1,), (1,)), ((), ())),
            precision=lax.Precision.HIGHEST, preferred_element_type=jnp.float32,
        )
        within = jnp.sum(base * parts[c], axis=0, keepdims=True)
        total = (every - within) * jnp.float32(sizes.scale[c])
        for h in range(2):
            result = jnp.where(row == 2 * c + h, total[:, h * LANES : (h + 1) * LANES], result)
    return charge[...] * result


def middle_kernel(sizes, boxes, own, mid, mass, charge, labels, send, own_out, mid_out,
                  packed, steps, targets, sums):
    force = force_of(boxes, own, charge, labels, packed, steps, targets, sums, sizes)
    kick = half_step * mass[...] * force
    midway = (mid[...] + kick) + kick
    places = own[...] + time_step * midway
    row = lax.broadcasted_iota(jnp.int32, (ROWS, LANES), 0)
    block = jnp.where(row < 6, places, own[...])
    own_out[...] = block
    mid_out[...] = midway
    for b in range(send.shape[0]):
        send[b] = block


def last_kernel(sizes, boxes, own, mid, mass, charge, labels, pos, vel, frc,
                packed, steps, targets, sums):
    force = force_of(boxes, own, charge, labels, packed, steps, targets, sums, sizes)
    velocity = mid[...] + half_step * mass[...] * force
    places = own[...]
    for c in range(3):
        for h in range(2):
            r = slice(2 * c + h, 2 * c + h + 1)
            cut = slice(h * LANES, (h + 1) * LANES)
            pos[c, 0, 0, :, cut] = places[r, :]
            vel[c, 0, 0, :, cut] = velocity[r, :]
            frc[c, 0, 0, :, cut] = force[r, :]


def cycle_offsets(cycle_size):
    if cycle_size >= 5:
        return [1, -1, 2, -2]
    return list(range(1, cycle_size))


def passed_along(block, axis, distance):
    devices = range(lax.axis_size(axis))
    route = [((i - distance) % len(devices), i) for i in devices]
    return lax.ppermute(block, axis, route)


def gather_near(copies, short, long):
    boxes = copies
    if short:
        boxes = lax.all_to_all(copies, short, 0, 0, tiled=True)
    for axis in long:
        pieces = [boxes]
        for offset in cycle_offsets(lax.axis_size(axis)):
            pieces.append(passed_along(boxes, axis, offset))
        boxes = jnp.concatenate(pieces)
    return boxes


def local(positions, velocities, forces, charges, inverse_mass, occupancy, molecule):
    axes = ("gx", "gy", "gz")
    extents = [lax.axis_size(axis) for axis in axes]
    sizes = Sizes([float(extent) for extent in extents])
    short = tuple(axis for axis, extent in zip(axes, extents) if extent < 5)
    long = tuple(axis for axis, extent in zip(axes, extents) if extent >= 5)
    copies = math.prod([1] + [extent for extent in extents if extent < 5])
    count = copies * 5 ** len(long)

    vmem = pl.BlockSpec(memory_space=pltpu.VMEM)
    smem = pl.BlockSpec(memory_space=pltpu.SMEM)
    block = jax.ShapeDtypeStruct((ROWS, LANES), jnp.float32)
    many = jax.ShapeDtypeStruct((copies, ROWS, LANES), jnp.float32)
    send, own, mid, mass, charge = pl.pallas_call(
        start_kernel,
        out_shape=(many, block, block, block, block),
        in_specs=[vmem] * 5 + [smem],
        out_specs=(vmem,) * 5,
        name="start",
    )(positions, velocities, forces, charges, inverse_mass, occupancy)

    scratch = [
        pltpu.VMEM((count + 1, ROWS, LANES), jnp.float32),
        pltpu.VMEM((count, ROWS, LANES), jnp.int32),
        pltpu.VMEM((3, 32, ROWS, LANES), jnp.int32),
        pltpu.VMEM((3, 2 * LANES, LANES), jnp.float32),
    ]
    boxes = gather_near(send, short, long)
    send, own, mid = pl.pallas_call(
        functools.partial(middle_kernel, sizes),
        out_shape=(many, block, block),
        in_specs=[vmem] * 6,
        out_specs=(vmem,) * 3,
        scratch_shapes=scratch,
        name="middle",
    )(boxes, own, mid, mass, charge, molecule)
    boxes = gather_near(send, short, long)
    whole = jax.ShapeDtypeStruct(positions.shape, jnp.float32)
    return pl.pallas_call(
        functools.partial(last_kernel, sizes),
        out_shape=(whole, whole, whole),
        in_specs=[vmem] * 6,
        out_specs=(vmem,) * 3,
        scratch_shapes=scratch,
        name="last",
    )(boxes, own, mid, mass, charge, molecule)


def solution(mesh):
    in_specs = (
        P(None, "gx", "gy", "gz", None),
        P(None, "gx", "gy", "gz", None),
        P(None, "gx", "gy", "gz", None),
        P("gx", "gy", "gz", None),
        P("gx", "gy", "gz", None),
        P("gx", "gy", "gz"),
        P("gx", "gy", "gz", None),
    )
    out_specs = (
        P(None, "gx", "gy", "gz", None),
        P(None, "gx", "gy", "gz", None),
        P(None, "gx", "gy", "gz", None),
    )
    return jax.shard_map(local, mesh=mesh, in_specs=in_specs, out_specs=out_specs, check_vma=False)
```

```python
import functools
import math

import jax
import jax.numpy as jnp
from jax import lax
from jax.experimental import pallas as pl
from jax.experimental.pallas import tpu as pltpu
from jax.sharding import PartitionSpec as P

cutoff_square = 4.0
soften_square = 0.25
time_step = 0.1
half_step = 0.05

LANES = 128
ROWS = 8
UNROLL = 2
TIE_SHIFT = 160
FULL = 4294967296.0


class Sizes:
    def __init__(self, lengths):
        self.lengths = lengths
        self.unit = max(set(lengths), key=lengths.count)
        step = self.unit / FULL
        self.top = cutoff_square / step**2
        self.soft = soften_square / step**2
        self.ratio = [(length / self.unit) ** 2 for length in lengths]
        self.scale = [
            (1.0 / (cutoff_square * cutoff_square)) * step * (length / FULL) for length in lengths
        ]
        self.shift = [TIE_SHIFT if length * length / 4 < cutoff_square else 0 for length in lengths]


def row_constant(values):
    row = lax.broadcasted_iota(jnp.int32, (ROWS, LANES), 0) // 2
    out = jnp.zeros((ROWS, LANES), jnp.float32)
    for c, value in enumerate(values):
        out = jnp.where(row == c, jnp.float32(value), out)
    return out


def to_steps(values, inverse):
    turns = values * inverse
    turns = turns - jnp.round(turns)
    turns = jnp.where(turns >= 0.5, -0.5, turns)
    return (turns * jnp.float32(FULL)).astype(jnp.int32)


def pair_weight(target, source, charge, sizes):
    parts = [(t - s).astype(jnp.float32) for t, s in zip(target, source)]
    squared = None
    for part, ratio in sorted(zip(parts, sizes.ratio), key=lambda item: item[1] != 1.0):
        square = part * part
        if ratio != 1.0:
            square = square * jnp.float32(ratio)
        squared = square if squared is None else squared + square
    switch = jnp.maximum(jnp.float32(sizes.top) - squared, 0.0)
    root = lax.rsqrt(squared + jnp.float32(sizes.soft))
    first = switch * root
    return parts, (first * first) * (root * charge)


def start_kernel(pos, vel, frc, chg, imass, lab, occ, send, own, mid, mass, charge, label,
                 pos_in, vel_in, frc_in, chg_in, imass_in, sems):
    copies = [
        pltpu.make_async_copy(source, target, sems.at[i])
        for i, (source, target) in enumerate(
            ((pos, pos_in), (vel, vel_in), (frc, frc_in), (chg, chg_in), (imass, imass_in), (lab, label))
        )
    ]
    for copy in copies:
        copy.start()
    for copy in copies:
        copy.wait()
    live = lax.broadcasted_iota(jnp.int32, (1, 2 * LANES), 1) < occ[0, 0, 0]
    live_charge = jnp.where(live, chg_in[0, 0], 0.0)
    inverse = imass_in[0, 0]
    for h in range(2):
        cut = slice(h * LANES, (h + 1) * LANES)
        for c in range(3):
            r = slice(2 * c + h, 2 * c + h + 1)
            midway = vel_in[c, 0, 0] + half_step * inverse * frc_in[c, 0, 0]
            places = pos_in[c, 0, 0] + time_step * midway
            own[r, :] = places[:, cut]
            mid[r, :] = midway[:, cut]
            mass[r, :] = inverse[:, cut]
            charge[r, :] = live_charge[:, cut]
        r = slice(6 + h, 7 + h)
        own[r, :] = live_charge[:, cut]
        mid[r, :] = jnp.zeros((1, LANES), jnp.float32)
        mass[r, :] = jnp.zeros((1, LANES), jnp.float32)
        charge[r, :] = jnp.zeros((1, LANES), jnp.float32)
    block = own[...]
    for b in range(send.shape[0]):
        send[b] = block


def pack_sources(boxes, charges, steps, packed, inverse):
    count = boxes.shape[0]
    lane = lax.broadcasted_iota(jnp.int32, (ROWS, LANES), 1)
    odd = lax.rem(lax.broadcasted_iota(jnp.int32, (ROWS, LANES), 0), 2) == 1
    filled = []
    for b in range(count):
        tail = boxes[b, 7:8, :]
        filled.append(jnp.max(jnp.where(tail != 0.0, lane[:1] + 1, 0)))
    position = jnp.int32(0)
    packed[0] = jnp.zeros((ROWS, LANES), jnp.float32)
    for b in range(count):
        tile = position // LANES
        begin = lax.rem(position, LANES)
        moved = pltpu.roll(boxes[b], begin, 1)
        packed[tile] = jnp.where(lane >= begin, moved, packed[tile])
        packed[tile + 1] = jnp.where(lane < begin, moved, 0.0)
        position = position + filled[b]
    tiles = (position + (LANES - 1)) // LANES
    for b in range(count):
        both = jnp.where(odd, packed[b], boxes[b])
        turned = to_steps(both, inverse)
        charges[b] = both
        steps[b] = turned
        charges[count + b] = pltpu.roll(both, ROWS - 1, 0)
        steps[count + b] = pltpu.roll(turned, ROWS - 1, 0)
    for extra in range(UNROLL):
        charges[count + tiles + extra] = jnp.zeros((ROWS, LANES), jnp.float32)
        steps[count + tiles + extra] = jnp.zeros((ROWS, LANES), jnp.int32)
    return count + tiles


def force_of(boxes, own, charge, labels, charges, steps, packed, targets, sums, sizes):
    inverse = row_constant([1.0 / length for length in sizes.lengths])
    tiles = pack_sources(boxes, charges, steps, packed, inverse)
    mine = to_steps(own[...], inverse)
    columns = jnp.transpose(mine)
    for c in range(3):
        for h in range(2):
            for g in range(16):
                column = columns[8 * g : 8 * g + 8, 2 * c + h : 2 * c + h + 1]
                targets[c, 16 * h + g] = jnp.broadcast_to(column, (ROWS, LANES)) + sizes.shift[c]

    for c in range(3):
        sums[c] = jnp.zeros(sums.shape[1:], jnp.float32)

    def over_sources(k, unused):
        taken = []
        for u in range(UNROLL):
            tile = k * UNROLL + u
            taken.append([
                jnp.broadcast_to(steps[tile, 2 * c : 2 * c + 1, :], (ROWS, LANES)) for c in range(3)
            ] + [jnp.broadcast_to(charges[tile, 6:7, :], (ROWS, LANES))])
        for g in range(32):
            target = [targets[c, g] for c in range(3)]
            added = [None] * 3
            for source in taken:
                parts, base = pair_weight(target, source[:3], source[3], sizes)
                for c in range(3):
                    product = base * parts[c]
                    added[c] = product if added[c] is None else added[c] + product
            for c in range(3):
                rows = slice(ROWS * g, ROWS * g + ROWS)
                sums[c, rows, :] = sums[c, rows, :] + added[c]
        return unused

    lax.fori_loop(0, (tiles + (UNROLL - 1)) // UNROLL, over_sources, 0)

    def spread(array):
        line = jnp.concatenate([array[0:1, :], array[1:2, :]], axis=1)
        return jnp.broadcast_to(line, (ROWS, 2 * LANES))

    def shifted(array):
        return pltpu.roll(pltpu.roll(array, 2 * LANES - 3, 1), 0, 1, stride=1, stride_axis=0)

    here = [spread(mine[2 * c : 2 * c + 2]) for c in range(3)]
    there = [shifted(array) for array in here]
    charge_there = shifted(spread(charge[0:2, :]))
    label = jnp.broadcast_to(labels[0, 0], (ROWS, 2 * LANES))
    slot = lax.broadcasted_iota(jnp.int32, (ROWS, 2 * LANES), 1)
    away = lax.broadcasted_iota(jnp.int32, (ROWS, 2 * LANES), 0)
    other = slot + 3 - away
    same = (shifted(label) == label) & (other >= 0) & (other < 2 * LANES) & (away < 7)
    here = [array + shift for array, shift in zip(here, sizes.shift)]
    parts, base = pair_weight(here, there, jnp.where(same, charge_there, 0.0), sizes)

    row = lax.broadcasted_iota(jnp.int32, (ROWS, LANES), 0)
    ones = jnp.ones((ROWS, LANES), jnp.float32)
    result = jnp.zeros((ROWS, LANES), jnp.float32)
    for c in range(3):
        every = lax.dot_general(
            ones, sums[c], (((1,), (1,)), ((), ())),
            precision=lax.Precision.HIGHEST, preferred_element_type=jnp.float32,
        )
        within = jnp.sum(base * parts[c], axis=0, keepdims=True)
        total = (every - within) * jnp.float32(sizes.scale[c])
        for h in range(2):
            result = jnp.where(row == 2 * c + h, total[:, h * LANES : (h + 1) * LANES], result)
    return charge[...] * result


def middle_kernel(sizes, boxes, own, mid, mass, charge, labels, send, own_out, mid_out,
                  charges, steps, packed, targets, sums):
    force = force_of(boxes, own, charge, labels, charges, steps, packed, targets, sums, sizes)
    kick = half_step * mass[...] * force
    midway = (mid[...] + kick) + kick
    places = own[...] + time_step * midway
    row = lax.broadcasted_iota(jnp.int32, (ROWS, LANES), 0)
    block = jnp.where(row < 6, places, own[...])
    own_out[...] = block
    mid_out[...] = midway
    for b in range(send.shape[0]):
        send[b] = block


def last_kernel(sizes, boxes, own, mid, mass, charge, labels, pos, vel, frc,
                charges, steps, packed, targets, sums):
    force = force_of(boxes, own, charge, labels, charges, steps, packed, targets, sums, sizes)
    velocity = mid[...] + half_step * mass[...] * force
    places = own[...]
    for c in range(3):
        for h in range(2):
            r = slice(2 * c + h, 2 * c + h + 1)
            cut = slice(h * LANES, (h + 1) * LANES)
            pos[c, 0, 0, :, cut] = places[r, :]
            vel[c, 0, 0, :, cut] = velocity[r, :]
            frc[c, 0, 0, :, cut] = force[r, :]


def cycle_offsets(cycle_size):
    if cycle_size >= 5:
        return [1, -1, 2, -2]
    return list(range(1, cycle_size))


def passed_along(block, axis, distance):
    devices = range(lax.axis_size(axis))
    route = [((i - distance) % len(devices), i) for i in devices]
    return lax.ppermute(block, axis, route)


def gather_near(copies, short, long):
    boxes = copies
    if short:
        boxes = lax.all_to_all(copies, short, 0, 0, tiled=True)
    for axis in long:
        pieces = [boxes]
        for offset in cycle_offsets(lax.axis_size(axis)):
            pieces.append(passed_along(boxes, axis, offset))
        boxes = jnp.concatenate(pieces)
    return boxes


def local(positions, velocities, forces, charges, inverse_mass, occupancy, molecule):
    axes = ("gx", "gy", "gz")
    extents = [lax.axis_size(axis) for axis in axes]
    sizes = Sizes([float(extent) for extent in extents])
    short = tuple(axis for axis, extent in zip(axes, extents) if extent < 5)
    long = tuple(axis for axis, extent in zip(axes, extents) if extent >= 5)
    copies = math.prod([1] + [extent for extent in extents if extent < 5])
    count = copies * 5 ** len(long)

    vmem = pl.BlockSpec(memory_space=pltpu.VMEM)
    smem = pl.BlockSpec(memory_space=pltpu.SMEM)
    small = pltpu.CompilerParams(vmem_limit_bytes=8 * 1024 * 1024)
    block = jax.ShapeDtypeStruct((ROWS, LANES), jnp.float32)
    many = jax.ShapeDtypeStruct((copies, ROWS, LANES), jnp.float32)
    send, own, mid, mass, charge, label = pl.pallas_call(
        start_kernel,
        out_shape=(many, block, block, block, block, jax.ShapeDtypeStruct(molecule.shape, jnp.int32)),
        in_specs=[pl.BlockSpec(memory_space=pltpu.HBM)] * 6 + [smem],
        out_specs=(vmem,) * 6,
        scratch_shapes=[
            pltpu.VMEM(array.shape, array.dtype)
            for array in (positions, velocities, forces, charges, inverse_mass)
        ]
        + [pltpu.SemaphoreType.DMA((6,))],
        compiler_params=small,
        name="start",
    )(*[pltpu.with_memory_space_constraint(array, pltpu.HBM) for array in (positions, velocities, forces, charges, inverse_mass, molecule)], occupancy)

    scratch = [
        pltpu.VMEM((2 * count + UNROLL, ROWS, LANES), jnp.float32),
        pltpu.VMEM((2 * count + UNROLL, ROWS, LANES), jnp.int32),
        pltpu.VMEM((count + 1, ROWS, LANES), jnp.float32),
        pltpu.VMEM((3, 32, ROWS, LANES), jnp.int32),
        pltpu.VMEM((3, 2 * LANES, LANES), jnp.float32),
    ]
    boxes = gather_near(send, short, long)
    send, own, mid = pl.pallas_call(
        functools.partial(middle_kernel, sizes),
        out_shape=(many, block, block),
        in_specs=[vmem] * 6,
        out_specs=(vmem,) * 3,
        scratch_shapes=scratch,
        compiler_params=small,
        name="middle",
    )(boxes, own, mid, mass, charge, label)
    boxes = gather_near(send, short, long)
    whole = jax.ShapeDtypeStruct(positions.shape, jnp.float32)
    return pl.pallas_call(
        functools.partial(last_kernel, sizes),
        out_shape=(whole, whole, whole),
        in_specs=[vmem] * 6,
        out_specs=(vmem,) * 3,
        scratch_shapes=scratch,
        compiler_params=small,
        name="last",
    )(boxes, own, mid, mass, charge, label)


def solution(mesh):
    in_specs = (
        P(None, "gx", "gy", "gz", None),
        P(None, "gx", "gy", "gz", None),
        P(None, "gx", "gy", "gz", None),
        P("gx", "gy", "gz", None),
        P("gx", "gy", "gz", None),
        P("gx", "gy", "gz"),
        P("gx", "gy", "gz", None),
    )
    out_specs = (
        P(None, "gx", "gy", "gz", None),
        P(None, "gx", "gy", "gz", None),
        P(None, "gx", "gy", "gz", None),
    )
    return jax.shard_map(local, mesh=mesh, in_specs=in_specs, out_specs=out_specs, check_vma=False)
```

```python
import functools
import math

import jax
import jax.numpy as jnp
from jax import lax
from jax.experimental import pallas as pl
from jax.experimental.pallas import tpu as pltpu
from jax.sharding import PartitionSpec as P

cutoff_square = 4.0
soften_square = 0.25
time_step = 0.1
half_step = 0.05

LANES = 128
ROWS = 8
TIES = (128, 191)
FULL = 4294967296.0


class Sizes:
    def __init__(self, lengths):
        self.lengths = lengths
        self.unit = max(set(lengths), key=lengths.count)
        step = self.unit / FULL
        self.top = cutoff_square / step**2
        self.soft = soften_square / step**2
        self.ratio = [(length / self.unit) ** 2 for length in lengths]
        self.scale = [
            (1.0 / (cutoff_square * cutoff_square)) * step * (length / FULL) for length in lengths
        ]
        self.seam = [length * length / 4 < cutoff_square for length in lengths]


def row_constant(values):
    row = lax.broadcasted_iota(jnp.int32, (ROWS, LANES), 0) // 2
    out = jnp.zeros((ROWS, LANES), jnp.float32)
    for c, value in enumerate(values):
        out = jnp.where(row == c, jnp.float32(value), out)
    return out


def to_steps(values, inverse):
    turns = values * inverse
    turns = turns - jnp.round(turns)
    turns = jnp.where(turns >= 0.5, -0.5, turns)
    return (turns * jnp.float32(FULL)).astype(jnp.int32)


def seam_shift(places, sizes):
    row = lax.broadcasted_iota(jnp.int32, (ROWS, LANES), 0) // 2
    shift = jnp.zeros((ROWS, LANES), jnp.int32)
    for c, length in enumerate(sizes.lengths):
        if sizes.seam[c]:
            near = jnp.where(jnp.abs(places) < length / 4, TIES[0], TIES[1])
            shift = jnp.where(row == c, near, shift)
    return shift


def pair_weight(target, source, charge, sizes):
    parts = [(t - s).astype(jnp.float32) for t, s in zip(target, source)]
    squared = None
    for part, ratio in sorted(zip(parts, sizes.ratio), key=lambda item: item[1] != 1.0):
        square = part * part
        if ratio != 1.0:
            square = square * jnp.float32(ratio)
        squared = square if squared is None else squared + square
    switch = jnp.maximum(jnp.float32(sizes.top) - squared, 0.0)
    root = lax.rsqrt(squared + jnp.float32(sizes.soft))
    first = switch * root
    return parts, (first * first) * (root * charge)


def start_kernel(pos, vel, frc, chg, imass, lab, occ, send, own, mid, mass, charge, label,
                 pos_in, vel_in, frc_in, chg_in, imass_in, sems):
    copies = [
        pltpu.make_async_copy(source, target, sems.at[i])
        for i, (source, target) in enumerate(
            ((pos, pos_in), (vel, vel_in), (frc, frc_in), (chg, chg_in), (imass, imass_in), (lab, label))
        )
    ]
    for copy in copies:
        copy.start()
    for copy in copies:
        copy.wait()
    live = lax.broadcasted_iota(jnp.int32, (1, 2 * LANES), 1) < occ[0, 0, 0]
    live_charge = jnp.where(live, chg_in[0, 0], 0.0)
    inverse = imass_in[0, 0]
    for h in range(2):
        cut = slice(h * LANES, (h + 1) * LANES)
        for c in range(3):
            r = slice(2 * c + h, 2 * c + h + 1)
            midway = vel_in[c, 0, 0] + half_step * inverse * frc_in[c, 0, 0]
            places = pos_in[c, 0, 0] + time_step * midway
            own[r, :] = places[:, cut]
            mid[r, :] = midway[:, cut]
            mass[r, :] = inverse[:, cut]
            charge[r, :] = live_charge[:, cut]
        r = slice(6 + h, 7 + h)
        own[r, :] = live_charge[:, cut]
        mid[r, :] = jnp.zeros((1, LANES), jnp.float32)
        mass[r, :] = jnp.zeros((1, LANES), jnp.float32)
        charge[r, :] = jnp.zeros((1, LANES), jnp.float32)
    block = own[...]
    for b in range(send.shape[0]):
        send[b] = block


def side_kernel(sizes, own, charge, labels, targets, band):
    mine = to_steps(own[...], row_constant([1.0 / length for length in sizes.lengths]))
    aim = mine + seam_shift(own[...], sizes)
    columns = jnp.transpose(aim)
    for c in range(3):
        for h in range(2):
            for g in range(LANES // ROWS):
                column = columns[ROWS * g : ROWS * g + ROWS, 2 * c + h : 2 * c + h + 1]
                spot = h * (LANES // ROWS) + g
                targets[c, spot] = jnp.broadcast_to(column, (ROWS, LANES))

    def spread(array):
        line = jnp.concatenate([array[0:1, :], array[1:2, :]], axis=1)
        return jnp.broadcast_to(line, (ROWS, 2 * LANES))

    def shifted(array):
        return pltpu.roll(pltpu.roll(array, 2 * LANES - 3, 1), 0, 1, stride=1, stride_axis=0)

    here = [spread(aim[2 * c : 2 * c + 2]) for c in range(3)]
    there = [shifted(spread(mine[2 * c : 2 * c + 2])) for c in range(3)]
    charge_there = shifted(spread(charge[0:2, :]))
    label = jnp.broadcast_to(labels[0, 0], (ROWS, 2 * LANES))
    slot = lax.broadcasted_iota(jnp.int32, (ROWS, 2 * LANES), 1)
    away = lax.broadcasted_iota(jnp.int32, (ROWS, 2 * LANES), 0)
    other = slot + 3 - away
    same = (shifted(label) == label) & (other >= 0) & (other < 2 * LANES) & (away < 7)
    parts, base = pair_weight(here, there, jnp.where(same, charge_there, 0.0), sizes)
    band[...] = jnp.zeros((ROWS, LANES), jnp.float32)
    for c in range(3):
        within = jnp.sum(base * parts[c], axis=0, keepdims=True)
        for h in range(2):
            band[2 * c + h : 2 * c + h + 1, :] = within[:, h * LANES : (h + 1) * LANES]


def add_tiles(tiles, targets, sums, sizes):
    for g in range(2 * LANES // ROWS):
        target = [targets[c, g] for c in range(3)]
        added = [None] * 3
        for source, charge in tiles:
            parts, base = pair_weight(target, source, charge, sizes)
            for c in range(3):
                product = base * parts[c]
                added[c] = product if added[c] is None else added[c] + product
        for c in range(3):
            rows = slice(ROWS * g, ROWS * g + ROWS)
            sums[c, rows, :] = sums[c, rows, :] + added[c]


def force_of(boxes, charge, band, targets, steps, packed, sums, sizes):
    count = boxes.shape[0]
    stride = 2 if count % 2 == 0 else 1
    inverse = row_constant([1.0 / length for length in sizes.lengths])
    lane = lax.broadcasted_iota(jnp.int32, (ROWS, LANES), 1)
    for c in range(3):
        sums[c] = jnp.zeros(sums.shape[1:], jnp.float32)
    packed[0] = jnp.zeros((ROWS, LANES), jnp.float32)

    def turned(source, first, target):
        for u in range(stride):
            steps[target + u] = to_steps(source[first + u], inverse)

    def taken(first, spot, source, half):
        return [
            (
                [
                    jnp.broadcast_to(
                        steps[spot + u, 2 * c + half : 2 * c + half + 1, :], (ROWS, LANES)
                    )
                    for c in range(3)
                ],
                jnp.broadcast_to(source[first + u, 6 + half : 7 + half, :], (ROWS, LANES)),
            )
            for u in range(stride)
        ]

    def heads(k, position):
        first = k * stride
        spot = lax.rem(k, 2) * stride
        add_tiles(taken(first, spot, boxes, 0), targets, sums, sizes)
        turned(boxes, jnp.minimum(first + stride, count - stride), stride - spot)
        for u in range(stride):
            box = boxes[first + u]
            filled = jnp.max(jnp.where(box[7:8, :] != 0.0, lane[:1] + 1, 0))
            tile = position // LANES
            begin = lax.rem(position, LANES)
            moved = pltpu.roll(box, begin, 1)
            packed[tile] = jnp.where(lane >= begin, moved, packed[tile])
            packed[tile + 1] = jnp.where(lane < begin, moved, 0.0)
            position = position + filled
        return position

    turned(boxes, 0, 0)
    position = lax.fori_loop(0, count // stride, heads, jnp.int32(0))
    tiles = (position + (LANES - 1)) // LANES
    for u in range(stride):
        packed[tiles + u] = jnp.zeros((ROWS, LANES), jnp.float32)

    def tails(k, unused):
        first = k * stride
        spot = lax.rem(k, 2) * stride
        add_tiles(taken(first, spot, packed, 1), targets, sums, sizes)
        turned(packed, first + stride, stride - spot)
        return unused

    turned(packed, 0, 0)
    lax.fori_loop(0, (tiles + stride - 1) // stride, tails, 0)

    row = lax.broadcasted_iota(jnp.int32, (ROWS, LANES), 0)
    ones = jnp.ones((ROWS, LANES), jnp.bfloat16)
    result = jnp.zeros((ROWS, LANES), jnp.float32)
    for c in range(3):
        left = sums[c]
        total = jnp.zeros((ROWS, 2 * LANES), jnp.float32)
        for piece in range(3):
            part = left.astype(jnp.bfloat16)
            left = left - part.astype(jnp.float32)
            total = total + lax.dot_general(
                ones, part, (((1,), (1,)), ((), ())), preferred_element_type=jnp.float32
            )
        for h in range(2):
            result = jnp.where(row == 2 * c + h, total[:, h * LANES : (h + 1) * LANES], result)
    return charge[...] * ((result - band[...]) * row_constant(sizes.scale))


def middle_kernel(sizes, boxes, own, mid, mass, charge, band, targets, send, own_out, mid_out,
                  steps, packed, sums):
    force = force_of(boxes, charge, band, targets, steps, packed, sums, sizes)
    kick = half_step * mass[...] * force
    midway = (mid[...] + kick) + kick
    places = own[...] + time_step * midway
    row = lax.broadcasted_iota(jnp.int32, (ROWS, LANES), 0)
    block = jnp.where(row < 6, places, own[...])
    own_out[...] = block
    mid_out[...] = midway
    for b in range(send.shape[0]):
        send[b] = block


def last_kernel(sizes, boxes, own, mid, mass, charge, band, targets, pos, vel, frc,
                steps, packed, sums):
    force = force_of(boxes, charge, band, targets, steps, packed, sums, sizes)
    velocity = mid[...] + half_step * mass[...] * force
    places = own[...]
    for c in range(3):
        for h in range(2):
            r = slice(2 * c + h, 2 * c + h + 1)
            cut = slice(h * LANES, (h + 1) * LANES)
            pos[c, 0, 0, :, cut] = places[r, :]
            vel[c, 0, 0, :, cut] = velocity[r, :]
            frc[c, 0, 0, :, cut] = force[r, :]


def cycle_offsets(cycle_size):
    if cycle_size >= 5:
        return [1, -1, 2, -2]
    return list(range(1, cycle_size))


def passed_along(block, axis, distance):
    devices = range(lax.axis_size(axis))
    route = [((i - distance) % len(devices), i) for i in devices]
    return lax.ppermute(block, axis, route)


def gather_near(copies, short, long):
    boxes = copies
    if short:
        boxes = lax.all_to_all(copies, short, 0, 0, tiled=True)
    for axis in long:
        pieces = [boxes]
        for offset in cycle_offsets(lax.axis_size(axis)):
            pieces.append(passed_along(boxes, axis, offset))
        boxes = jnp.concatenate(pieces)
    return boxes


def local(positions, velocities, forces, charges, inverse_mass, occupancy, molecule):
    axes = ("gx", "gy", "gz")
    extents = [lax.axis_size(axis) for axis in axes]
    sizes = Sizes([float(extent) for extent in extents])
    short = tuple(axis for axis, extent in zip(axes, extents) if extent < 5)
    long = tuple(axis for axis, extent in zip(axes, extents) if extent >= 5)
    copies = math.prod([1] + [extent for extent in extents if extent < 5])
    count = copies * 5 ** len(long)

    vmem = pl.BlockSpec(memory_space=pltpu.VMEM)
    smem = pl.BlockSpec(memory_space=pltpu.SMEM)
    small = pltpu.CompilerParams(vmem_limit_bytes=8 * 1024 * 1024)
    block = jax.ShapeDtypeStruct((ROWS, LANES), jnp.float32)
    many = jax.ShapeDtypeStruct((copies, ROWS, LANES), jnp.float32)
    send, own, mid, mass, charge, label = pl.pallas_call(
        start_kernel,
        out_shape=(many, block, block, block, block, jax.ShapeDtypeStruct(molecule.shape, jnp.int32)),
        in_specs=[pl.BlockSpec(memory_space=pltpu.HBM)] * 6 + [smem],
        out_specs=(vmem,) * 6,
        scratch_shapes=[
            pltpu.VMEM(array.shape, array.dtype)
            for array in (positions, velocities, forces, charges, inverse_mass)
        ]
        + [pltpu.SemaphoreType.DMA((6,))],
        compiler_params=small,
        name="start",
    )(*[pltpu.with_memory_space_constraint(array, pltpu.HBM) for array in (positions, velocities, forces, charges, inverse_mass, molecule)], occupancy)

    pairs = 2 * LANES * LANES * 2 * count
    scratch = [
        pltpu.VMEM((4, ROWS, LANES), jnp.int32),
        pltpu.VMEM((count + 4, ROWS, LANES), jnp.float32),
        pltpu.VMEM((3, 2 * LANES, LANES), jnp.float32),
    ]
    cost = pl.CostEstimate(flops=26 * pairs, bytes_accessed=64 * pairs // LANES, transcendentals=pairs)

    def beside(own):
        return pl.pallas_call(
            functools.partial(side_kernel, sizes),
            out_shape=(jax.ShapeDtypeStruct((3, 2 * LANES // ROWS, ROWS, LANES), jnp.int32), block),
            in_specs=[vmem] * 3,
            out_specs=(vmem,) * 2,
            compiler_params=small,
            cost_estimate=pl.CostEstimate(flops=4_000_000, bytes_accessed=400_000, transcendentals=2048),
            name="side",
        )(own, charge, label)

    targets, band = beside(own)
    boxes = gather_near(send, short, long)
    send, own, mid = pl.pallas_call(
        functools.partial(middle_kernel, sizes),
        out_shape=(many, block, block),
        in_specs=[vmem] * 7,
        out_specs=(vmem,) * 3,
        scratch_shapes=scratch,
        compiler_params=small,
        cost_estimate=cost,
        name="middle",
    )(boxes, own, mid, mass, charge, band, targets)
    targets, band = beside(own)
    boxes = gather_near(send, short, long)
    whole = jax.ShapeDtypeStruct(positions.shape, jnp.float32)
    return pl.pallas_call(
        functools.partial(last_kernel, sizes),
        out_shape=(whole, whole, whole),
        in_specs=[vmem] * 7,
        out_specs=(vmem,) * 3,
        scratch_shapes=scratch,
        compiler_params=small,
        cost_estimate=cost,
        name="last",
    )(boxes, own, mid, mass, charge, band, targets)


def solution(mesh):
    in_specs = (
        P(None, "gx", "gy", "gz", None),
        P(None, "gx", "gy", "gz", None),
        P(None, "gx", "gy", "gz", None),
        P("gx", "gy", "gz", None),
        P("gx", "gy", "gz", None),
        P("gx", "gy", "gz"),
        P("gx", "gy", "gz", None),
    )
    out_specs = (
        P(None, "gx", "gy", "gz", None),
        P(None, "gx", "gy", "gz", None),
        P(None, "gx", "gy", "gz", None),
    )
    return jax.shard_map(local, mesh=mesh, in_specs=in_specs, out_specs=out_specs, check_vma=False)
```

```python
import functools
import math

import jax
import jax.numpy as jnp
from jax import lax
from jax.experimental import pallas as pl
from jax.experimental.pallas import tpu as pltpu
from jax.sharding import PartitionSpec as P

cutoff_square = 4.0
soften_square = 0.25
time_step = 0.1
half_step = 0.05

LANES = 128
ROWS = 8
TIES = (128, 191)
FULL = 4294967296.0


class Sizes:
    def __init__(self, lengths):
        self.lengths = lengths
        self.unit = max(set(lengths), key=lengths.count)
        step = self.unit / FULL
        self.top = cutoff_square / step**2
        self.soft = soften_square / step**2
        self.ratio = [(length / self.unit) ** 2 for length in lengths]
        self.scale = [
            (1.0 / (cutoff_square * cutoff_square)) * step * (length / FULL) for length in lengths
        ]
        self.seam = [length * length / 4 < cutoff_square for length in lengths]


def row_constant(values):
    row = lax.broadcasted_iota(jnp.int32, (ROWS, LANES), 0) // 2
    out = jnp.zeros((ROWS, LANES), jnp.float32)
    for c, value in enumerate(values):
        out = jnp.where(row == c, jnp.float32(value), out)
    return out


def to_steps(values, inverse):
    turns = values * inverse
    turns = turns - jnp.round(turns)
    turns = jnp.where(turns >= 0.5, -0.5, turns)
    return (turns * jnp.float32(FULL)).astype(jnp.int32)


def seam_shift(places, sizes):
    row = lax.broadcasted_iota(jnp.int32, (ROWS, LANES), 0) // 2
    shift = jnp.zeros((ROWS, LANES), jnp.int32)
    for c, length in enumerate(sizes.lengths):
        if sizes.seam[c]:
            near = jnp.where(jnp.abs(places) < length / 4, TIES[0], TIES[1])
            shift = jnp.where(row == c, near, shift)
    return shift


def pair_weight(target, source, charge, sizes):
    parts = [(t - s).astype(jnp.float32) for t, s in zip(target, source)]
    squared = None
    for part, ratio in sorted(zip(parts, sizes.ratio), key=lambda item: item[1] != 1.0):
        square = part * part
        if ratio != 1.0:
            square = square * jnp.float32(ratio)
        squared = square if squared is None else squared + square
    switch = jnp.maximum(jnp.float32(sizes.top) - squared, 0.0)
    root = lax.rsqrt(squared + jnp.float32(sizes.soft))
    first = switch * root
    return parts, (first * first) * (root * charge)


def start_kernel(pos, vel, frc, chg, imass, lab, occ, send, own, mid, mass, charge, label,
                 pos_in, vel_in, frc_in, chg_in, imass_in, sems):
    copies = [
        pltpu.make_async_copy(source, target, sems.at[i])
        for i, (source, target) in enumerate(
            ((pos, pos_in), (vel, vel_in), (frc, frc_in), (chg, chg_in), (imass, imass_in), (lab, label))
        )
    ]
    for copy in copies:
        copy.start()
    for copy in copies:
        copy.wait()
    live = lax.broadcasted_iota(jnp.int32, (1, 2 * LANES), 1) < occ[0, 0, 0]
    live_charge = jnp.where(live, chg_in[0, 0], 0.0)
    inverse = imass_in[0, 0]
    for h in range(2):
        cut = slice(h * LANES, (h + 1) * LANES)
        for c in range(3):
            r = slice(2 * c + h, 2 * c + h + 1)
            midway = vel_in[c, 0, 0] + half_step * inverse * frc_in[c, 0, 0]
            places = pos_in[c, 0, 0] + time_step * midway
            own[r, :] = places[:, cut]
            mid[r, :] = midway[:, cut]
            mass[r, :] = inverse[:, cut]
            charge[r, :] = live_charge[:, cut]
        r = slice(6 + h, 7 + h)
        own[r, :] = live_charge[:, cut]
        mid[r, :] = jnp.zeros((1, LANES), jnp.float32)
        mass[r, :] = jnp.zeros((1, LANES), jnp.float32)
        charge[r, :] = jnp.zeros((1, LANES), jnp.float32)
    block = own[...]
    for b in range(send.shape[0]):
        send[b] = block


def prepare(own, charge, labels, targets, sizes):
    mine = to_steps(own[...], row_constant([1.0 / length for length in sizes.lengths]))
    aim = mine + seam_shift(own[...], sizes)
    columns = jnp.transpose(aim)
    for c in range(3):
        for h in range(2):
            for g in range(LANES // ROWS):
                column = columns[ROWS * g : ROWS * g + ROWS, 2 * c + h : 2 * c + h + 1]
                spot = h * (LANES // ROWS) + g
                targets[c, spot] = jnp.broadcast_to(column, (ROWS, LANES))

    def spread(array):
        line = jnp.concatenate([array[0:1, :], array[1:2, :]], axis=1)
        return jnp.broadcast_to(line, (ROWS, 2 * LANES))

    def shifted(array):
        return pltpu.roll(pltpu.roll(array, 2 * LANES - 3, 1), 0, 1, stride=1, stride_axis=0)

    here = [spread(aim[2 * c : 2 * c + 2]) for c in range(3)]
    there = [shifted(spread(mine[2 * c : 2 * c + 2])) for c in range(3)]
    charge_there = shifted(spread(charge[0:2, :]))
    label = jnp.broadcast_to(labels[0, 0], (ROWS, 2 * LANES))
    slot = lax.broadcasted_iota(jnp.int32, (ROWS, 2 * LANES), 1)
    away = lax.broadcasted_iota(jnp.int32, (ROWS, 2 * LANES), 0)
    other = slot + 3 - away
    same = (shifted(label) == label) & (other >= 0) & (other < 2 * LANES) & (away < 7)
    parts, base = pair_weight(here, there, jnp.where(same, charge_there, 0.0), sizes)
    return [jnp.sum(base * parts[c], axis=0, keepdims=True) for c in range(3)]


def add_tiles(tiles, targets, sums, sizes):
    for g in range(2 * LANES // ROWS):
        target = [targets[c, g] for c in range(3)]
        added = [None] * 3
        for source, charge in tiles:
            parts, base = pair_weight(target, source, charge, sizes)
            for c in range(3):
                product = base * parts[c]
                added[c] = product if added[c] is None else added[c] + product
        for c in range(3):
            rows = slice(ROWS * g, ROWS * g + ROWS)
            sums[c, rows, :] = sums[c, rows, :] + added[c]


def force_of(boxes, own, charge, labels, steps, packed, offsets, targets, sums, sizes):
    count = boxes.shape[0]
    stride = 2 if count % 2 == 0 else 1
    inverse = row_constant([1.0 / length for length in sizes.lengths])
    lane = lax.broadcasted_iota(jnp.int32, (ROWS, LANES), 1)
    within = prepare(own, charge, labels, targets, sizes)
    for c in range(3):
        sums[c] = jnp.zeros(sums.shape[1:], jnp.float32)
    packed[0] = jnp.zeros((ROWS, LANES), jnp.float32)

    def turned(source, first, target):
        for u in range(stride):
            steps[target + u] = to_steps(source[first + u], inverse)

    def taken(first, spot, source, half):
        return [
            (
                [
                    jnp.broadcast_to(
                        steps[spot + u, 2 * c + half : 2 * c + half + 1, :], (ROWS, LANES)
                    )
                    for c in range(3)
                ],
                jnp.broadcast_to(source[first + u, 6 + half : 7 + half, :], (ROWS, LANES)),
            )
            for u in range(stride)
        ]

    def heads(k, unused):
        first = k * stride
        spot = lax.rem(k, 2) * stride
        add_tiles(taken(first, spot, boxes, 0), targets, sums, sizes)
        turned(boxes, jnp.minimum(first + stride, count - stride), stride - spot)
        for u in range(stride):
            box = boxes[first + u]
            position = offsets[first + u]
            tile = position // LANES
            begin = lax.rem(position, LANES)
            moved = pltpu.roll(box, begin, 1)
            pltpu.store(packed.at[tile], moved, mask=lane >= begin)
            packed[tile + 1] = jnp.where(lane < begin, moved, 0.0)
        return unused

    turned(boxes, 0, 0)
    position = jnp.int32(0)
    last_live = jnp.max(jnp.where(boxes[:, 7, :] != 0.0, lane[:1].astype(jnp.float32) + 1.0, 0.0), axis=1, keepdims=True)
    filled = last_live.astype(jnp.int32)
    for b in range(count):
        offsets[b] = position
        position = position + filled[b, 0]
    lax.fori_loop(0, count // stride, heads, 0)
    tiles = (position + (LANES - 1)) // LANES
    for u in range(stride):
        packed[tiles + u] = jnp.zeros((ROWS, LANES), jnp.float32)

    def tails(k, unused):
        first = k * stride
        spot = lax.rem(k, 2) * stride
        add_tiles(taken(first, spot, packed, 1), targets, sums, sizes)
        turned(packed, first + stride, stride - spot)
        return unused

    turned(packed, 0, 0)
    lax.fori_loop(0, (tiles + stride - 1) // stride, tails, 0)

    row = lax.broadcasted_iota(jnp.int32, (ROWS, LANES), 0)
    ones = jnp.ones((ROWS, LANES), jnp.bfloat16)
    result = jnp.zeros((ROWS, LANES), jnp.float32)
    for c in range(3):
        left = sums[c]
        total = jnp.zeros((ROWS, 2 * LANES), jnp.float32)
        for piece in range(3):
            part = left.astype(jnp.bfloat16)
            left = left - part.astype(jnp.float32)
            total = total + lax.dot_general(
                ones, part, (((1,), (1,)), ((), ())), preferred_element_type=jnp.float32
            )
        total = (total - within[c]) * jnp.float32(sizes.scale[c])
        for h in range(2):
            result = jnp.where(row == 2 * c + h, total[:, h * LANES : (h + 1) * LANES], result)
    return charge[...] * result


def middle_kernel(sizes, boxes, own, mid, mass, charge, labels, send, own_out, mid_out,
                  steps, packed, offsets, targets, sums):
    force = force_of(boxes, own, charge, labels, steps, packed, offsets, targets, sums, sizes)
    kick = half_step * mass[...] * force
    midway = (mid[...] + kick) + kick
    places = own[...] + time_step * midway
    row = lax.broadcasted_iota(jnp.int32, (ROWS, LANES), 0)
    block = jnp.where(row < 6, places, own[...])
    own_out[...] = block
    mid_out[...] = midway
    for b in range(send.shape[0]):
        send[b] = block


def last_kernel(sizes, boxes, own, mid, mass, charge, labels, pos, vel, frc,
                steps, packed, offsets, targets, sums):
    force = force_of(boxes, own, charge, labels, steps, packed, offsets, targets, sums, sizes)
    velocity = mid[...] + half_step * mass[...] * force
    places = own[...]
    for c in range(3):
        for h in range(2):
            r = slice(2 * c + h, 2 * c + h + 1)
            cut = slice(h * LANES, (h + 1) * LANES)
            pos[c, 0, 0, :, cut] = places[r, :]
            vel[c, 0, 0, :, cut] = velocity[r, :]
            frc[c, 0, 0, :, cut] = force[r, :]


def cycle_offsets(cycle_size):
    if cycle_size >= 5:
        return [1, -1, 2, -2]
    return list(range(1, cycle_size))


def passed_along(block, axis, distance):
    devices = range(lax.axis_size(axis))
    route = [((i - distance) % len(devices), i) for i in devices]
    return lax.ppermute(block, axis, route)


def gather_near(copies, short, long):
    boxes = copies
    if short:
        boxes = lax.all_to_all(copies, short, 0, 0, tiled=True)
    for axis in long:
        pieces = [boxes]
        for offset in cycle_offsets(lax.axis_size(axis)):
            pieces.append(passed_along(boxes, axis, offset))
        boxes = jnp.concatenate(pieces)
    return boxes


def local(positions, velocities, forces, charges, inverse_mass, occupancy, molecule):
    axes = ("gx", "gy", "gz")
    extents = [lax.axis_size(axis) for axis in axes]
    sizes = Sizes([float(extent) for extent in extents])
    short = tuple(axis for axis, extent in zip(axes, extents) if extent < 5)
    long = tuple(axis for axis, extent in zip(axes, extents) if extent >= 5)
    copies = math.prod([1] + [extent for extent in extents if extent < 5])
    count = copies * 5 ** len(long)

    vmem = pl.BlockSpec(memory_space=pltpu.VMEM)
    smem = pl.BlockSpec(memory_space=pltpu.SMEM)
    small = pltpu.CompilerParams(vmem_limit_bytes=8 * 1024 * 1024)
    block = jax.ShapeDtypeStruct((ROWS, LANES), jnp.float32)
    many = jax.ShapeDtypeStruct((copies, ROWS, LANES), jnp.float32)
    send, own, mid, mass, charge, label = pl.pallas_call(
        start_kernel,
        out_shape=(many, block, block, block, block, jax.ShapeDtypeStruct(molecule.shape, jnp.int32)),
        in_specs=[pl.BlockSpec(memory_space=pltpu.HBM)] * 6 + [smem],
        out_specs=(vmem,) * 6,
        scratch_shapes=[
            pltpu.VMEM(array.shape, array.dtype)
            for array in (positions, velocities, forces, charges, inverse_mass)
        ]
        + [pltpu.SemaphoreType.DMA((6,))],
        compiler_params=small,
        name="start",
    )(*[pltpu.with_memory_space_constraint(array, pltpu.HBM) for array in (positions, velocities, forces, charges, inverse_mass, molecule)], occupancy)

    pairs = 2 * LANES * LANES * 2 * count
    scratch = [
        pltpu.VMEM((4, ROWS, LANES), jnp.int32),
        pltpu.VMEM((count + 4, ROWS, LANES), jnp.float32),
        pltpu.SMEM((count,), jnp.int32),
        pltpu.VMEM((3, 2 * LANES // ROWS, ROWS, LANES), jnp.int32),
        pltpu.VMEM((3, 2 * LANES, LANES), jnp.float32),
    ]
    cost = pl.CostEstimate(flops=26 * pairs, bytes_accessed=64 * pairs // LANES, transcendentals=pairs)

    boxes = gather_near(send, short, long)
    send, own, mid = pl.pallas_call(
        functools.partial(middle_kernel, sizes),
        out_shape=(many, block, block),
        in_specs=[vmem] * 6,
        out_specs=(vmem,) * 3,
        scratch_shapes=scratch,
        compiler_params=small,
        cost_estimate=cost,
        name="middle",
    )(boxes, own, mid, mass, charge, label)
    boxes = gather_near(send, short, long)
    whole = jax.ShapeDtypeStruct(positions.shape, jnp.float32)
    return pl.pallas_call(
        functools.partial(last_kernel, sizes),
        out_shape=(whole, whole, whole),
        in_specs=[vmem] * 6,
        out_specs=(vmem,) * 3,
        scratch_shapes=scratch,
        compiler_params=small,
        cost_estimate=cost,
        name="last",
    )(boxes, own, mid, mass, charge, label)


def solution(mesh):
    in_specs = (
        P(None, "gx", "gy", "gz", None),
        P(None, "gx", "gy", "gz", None),
        P(None, "gx", "gy", "gz", None),
        P("gx", "gy", "gz", None),
        P("gx", "gy", "gz", None),
        P("gx", "gy", "gz"),
        P("gx", "gy", "gz", None),
    )
    out_specs = (
        P(None, "gx", "gy", "gz", None),
        P(None, "gx", "gy", "gz", None),
        P(None, "gx", "gy", "gz", None),
    )
    return jax.shard_map(local, mesh=mesh, in_specs=in_specs, out_specs=out_specs, check_vma=False)
```

```python
import functools
import math

import jax
import jax.numpy as jnp
from jax import lax
from jax.experimental import pallas as pl
from jax.experimental.pallas import tpu as pltpu
from jax.sharding import PartitionSpec as P

cutoff_square = 4.0
soften_square = 0.25
time_step = 0.1
half_step = 0.05

LANES = 128
ROWS = 8
TIES = (128, 191)
FULL = 4294967296.0


class Sizes:
    def __init__(self, lengths):
        self.lengths = lengths
        self.unit = max(set(lengths), key=lengths.count)
        step = self.unit / FULL
        self.top = cutoff_square / step**2
        self.soft = soften_square / step**2
        self.ratio = [(length / self.unit) ** 2 for length in lengths]
        self.scale = [
            (1.0 / (cutoff_square * cutoff_square)) * step * (length / FULL) for length in lengths
        ]
        self.seam = [length * length / 4 < cutoff_square for length in lengths]


def row_constant(values):
    row = lax.broadcasted_iota(jnp.int32, (ROWS, LANES), 0) // 2
    out = jnp.zeros((ROWS, LANES), jnp.float32)
    for c, value in enumerate(values):
        out = jnp.where(row == c, jnp.float32(value), out)
    return out


def to_steps(values, inverse):
    turns = values * inverse
    turns = turns - jnp.round(turns)
    turns = jnp.where(turns >= 0.5, -0.5, turns)
    return (turns * jnp.float32(FULL)).astype(jnp.int32)


def seam_shift(places, sizes):
    row = lax.broadcasted_iota(jnp.int32, (ROWS, LANES), 0) // 2
    shift = jnp.zeros((ROWS, LANES), jnp.int32)
    for c, length in enumerate(sizes.lengths):
        if sizes.seam[c]:
            near = jnp.where(jnp.abs(places) < length / 4, TIES[0], TIES[1])
            shift = jnp.where(row == c, near, shift)
    return shift


def pair_weight(target, source, charge, sizes):
    parts = [(t - s).astype(jnp.float32) for t, s in zip(target, source)]
    squared = None
    for part, ratio in sorted(zip(parts, sizes.ratio), key=lambda item: item[1] != 1.0):
        square = part * part
        if ratio != 1.0:
            square = square * jnp.float32(ratio)
        squared = square if squared is None else squared + square
    switch = jnp.maximum(jnp.float32(sizes.top) - squared, 0.0)
    root = lax.rsqrt(squared + jnp.float32(sizes.soft))
    first = switch * root
    return parts, (first * first) * (root * charge)


def start_kernel(pos, vel, frc, chg, imass, lab, occ, send, own, mid, mass, charge, label,
                 pos_in, vel_in, frc_in, chg_in, imass_in, sems):
    copies = [
        pltpu.make_async_copy(source, target, sems.at[i])
        for i, (source, target) in enumerate(
            ((pos, pos_in), (vel, vel_in), (frc, frc_in), (chg, chg_in), (imass, imass_in), (lab, label))
        )
    ]
    for copy in copies:
        copy.start()
    for copy in copies:
        copy.wait()
    live = lax.broadcasted_iota(jnp.int32, (1, 2 * LANES), 1) < occ[0, 0, 0]
    live_charge = jnp.where(live, chg_in[0, 0], 0.0)
    inverse = imass_in[0, 0]
    for h in range(2):
        cut = slice(h * LANES, (h + 1) * LANES)
        for c in range(3):
            r = slice(2 * c + h, 2 * c + h + 1)
            midway = vel_in[c, 0, 0] + half_step * inverse * frc_in[c, 0, 0]
            places = pos_in[c, 0, 0] + time_step * midway
            own[r, :] = places[:, cut]
            mid[r, :] = midway[:, cut]
            mass[r, :] = inverse[:, cut]
            charge[r, :] = live_charge[:, cut]
        r = slice(6 + h, 7 + h)
        own[r, :] = live_charge[:, cut]
        mid[r, :] = jnp.zeros((1, LANES), jnp.float32)
        mass[r, :] = jnp.zeros((1, LANES), jnp.float32)
        charge[r, :] = jnp.zeros((1, LANES), jnp.float32)
    block = own[...]
    for b in range(send.shape[0]):
        send[b] = block


def prepare(own, charge, labels, targets, sizes):
    mine = to_steps(own[...], row_constant([1.0 / length for length in sizes.lengths]))
    aim = mine + seam_shift(own[...], sizes)
    columns = jnp.transpose(aim)
    for c in range(3):
        for h in range(2):
            for g in range(LANES // ROWS):
                column = columns[ROWS * g : ROWS * g + ROWS, 2 * c + h : 2 * c + h + 1]
                spot = h * (LANES // ROWS) + g
                targets[c, spot] = jnp.broadcast_to(column, (ROWS, LANES))

    def spread(array):
        line = jnp.concatenate([array[0:1, :], array[1:2, :]], axis=1)
        return jnp.broadcast_to(line, (ROWS, 2 * LANES))

    def shifted(array):
        return pltpu.roll(pltpu.roll(array, 2 * LANES - 3, 1), 0, 1, stride=1, stride_axis=0)

    here = [spread(aim[2 * c : 2 * c + 2]) for c in range(3)]
    there = [shifted(spread(mine[2 * c : 2 * c + 2])) for c in range(3)]
    charge_there = shifted(spread(charge[0:2, :]))
    label = jnp.broadcast_to(labels[0, 0], (ROWS, 2 * LANES))
    slot = lax.broadcasted_iota(jnp.int32, (ROWS, 2 * LANES), 1)
    away = lax.broadcasted_iota(jnp.int32, (ROWS, 2 * LANES), 0)
    other = slot + 3 - away
    same = (shifted(label) == label) & (other >= 0) & (other < 2 * LANES) & (away < 7)
    parts, base = pair_weight(here, there, jnp.where(same, charge_there, 0.0), sizes)
    return [jnp.sum(base * parts[c], axis=0, keepdims=True) for c in range(3)]


def add_tiles(tiles, targets, sums, sizes):
    for g in range(2 * LANES // ROWS):
        target = [targets[c, g] for c in range(3)]
        added = [None] * 3
        for source, charge in tiles:
            parts, base = pair_weight(target, source, charge, sizes)
            for c in range(3):
                product = base * parts[c]
                added[c] = product if added[c] is None else added[c] + product
        for c in range(3):
            rows = slice(ROWS * g, ROWS * g + ROWS)
            sums[c, rows, :] = sums[c, rows, :] + added[c]


def force_of(charges, places, per, own, charge, labels, steps, packed, packed_charges, offsets,
             targets, sums, sizes):
    count = charges.shape[0] // ROWS
    stride = 2 if count % 2 == 0 else 1
    lane = lax.broadcasted_iota(jnp.int32, (ROWS, LANES), 1)
    within = prepare(own, charge, labels, targets, sizes)
    for c in range(3):
        sums[c] = jnp.zeros(sums.shape[1:], jnp.float32)

    inverses = {}
    for k in range(pl.cdiv(places.shape[0], ROWS)):
        begin = (ROWS * k) % per
        if begin not in inverses:
            axis = lax.rem(lax.broadcasted_iota(jnp.int32, (ROWS, LANES), 0) + begin, per) // 2
            inverse = jnp.zeros((ROWS, LANES), jnp.float32)
            for c, length in enumerate(sizes.lengths):
                inverse = jnp.where(axis == c, jnp.float32(1.0 / length), inverse)
            inverses[begin] = inverse
        size = min(ROWS, places.shape[0] - ROWS * k)
        rows = slice(ROWS * k, ROWS * k + size)
        steps[rows, :] = to_steps(places[rows, :], inverses[begin][:size])

    def one(ref, row):
        return jnp.broadcast_to(ref[pl.ds(row, 1), :], (ROWS, LANES))

    def heads(k, unused):
        boxes = [k * stride + u for u in range(stride)]
        tiles = [
            ([one(steps, b * per + 2 * c) for c in range(3)], one(charges, b * ROWS + 6))
            for b in boxes
        ]
        add_tiles(tiles, targets, sums, sizes)
        for b in boxes:
            position = offsets[b]
            tile = position // LANES
            begin = lax.rem(position, LANES)
            late = lane >= begin
            moved = pltpu.roll(steps[pl.ds(b * per, ROWS), :], begin, 1)
            pltpu.store(packed.at[tile], moved, mask=late)
            packed[tile + 1] = moved
            box = charges[pl.ds(pl.multiple_of(b * ROWS, ROWS), ROWS), :]
            moved = pltpu.roll(box, begin, 1)
            pltpu.store(packed_charges.at[tile], moved, mask=late)
            packed_charges[tile + 1] = jnp.where(late, 0.0, moved)
        return unused

    live = jnp.where(
        charges[pl.ds(7, count, stride=ROWS), :] != 0.0, lane[:1].astype(jnp.float32) + 1.0, 0.0
    )
    filled = jnp.max(live, axis=1, keepdims=True).astype(jnp.int32)
    position = jnp.int32(0)
    for b in range(count):
        offsets[b] = position
        position = position + filled[b, 0]
    lax.fori_loop(0, count // stride, heads, 0)
    filled_tiles = (position + (LANES - 1)) // LANES
    for u in range(stride):
        packed_charges[filled_tiles + u] = jnp.zeros((ROWS, LANES), jnp.float32)

    def tails(k, unused):
        tiles = [
            (
                [
                    jnp.broadcast_to(packed[t, 2 * c + 1 : 2 * c + 2, :], (ROWS, LANES))
                    for c in range(3)
                ],
                jnp.broadcast_to(packed_charges[t, 7:8, :], (ROWS, LANES)),
            )
            for t in [k * stride + u for u in range(stride)]
        ]
        add_tiles(tiles, targets, sums, sizes)
        return unused

    lax.fori_loop(0, (filled_tiles + stride - 1) // stride, tails, 0)

    row = lax.broadcasted_iota(jnp.int32, (ROWS, LANES), 0)
    ones = jnp.ones((ROWS, LANES), jnp.bfloat16)
    result = jnp.zeros((ROWS, LANES), jnp.float32)
    for c in range(3):
        left = sums[c]
        total = jnp.zeros((ROWS, 2 * LANES), jnp.float32)
        for piece in range(3):
            part = left.astype(jnp.bfloat16)
            left = left - part.astype(jnp.float32)
            total = total + lax.dot_general(
                ones, part, (((1,), (1,)), ((), ())), preferred_element_type=jnp.float32
            )
        total = (total - within[c]) * jnp.float32(sizes.scale[c])
        for h in range(2):
            result = jnp.where(row == 2 * c + h, total[:, h * LANES : (h + 1) * LANES], result)
    return charge[...] * result


def middle_kernel(sizes, boxes, own, mid, mass, charge, labels, send, own_out, mid_out, *scratch):
    force = force_of(boxes, boxes, ROWS, own, charge, labels, *scratch, sizes)
    kick = half_step * mass[...] * force
    midway = (mid[...] + kick) + kick
    places = own[...] + time_step * midway
    row = lax.broadcasted_iota(jnp.int32, (ROWS, LANES), 0)
    block = jnp.where(row < 6, places, own[...])
    own_out[...] = block
    mid_out[...] = midway
    rows = send.shape[0]
    for k in range(pl.cdiv(rows, ROWS)):
        begin = (ROWS * k) % 6
        early = block if begin == 0 else pltpu.roll(block, ROWS - begin, 0)
        late = pltpu.roll(block, (6 - begin) % ROWS, 0)
        twice = jnp.where(row < 6 - begin, early, late)
        size = min(ROWS, rows - ROWS * k)
        send[ROWS * k : ROWS * k + size, :] = twice[:size]


def last_kernel(sizes, boxes, places_in, own, mid, mass, charge, labels, pos, vel, frc, *scratch):
    force = force_of(boxes, places_in, 6, own, charge, labels, *scratch, sizes)
    velocity = mid[...] + half_step * mass[...] * force
    places = own[...]
    for c in range(3):
        for h in range(2):
            r = slice(2 * c + h, 2 * c + h + 1)
            cut = slice(h * LANES, (h + 1) * LANES)
            pos[c, 0, 0, :, cut] = places[r, :]
            vel[c, 0, 0, :, cut] = velocity[r, :]
            frc[c, 0, 0, :, cut] = force[r, :]


def cycle_offsets(cycle_size):
    if cycle_size >= 5:
        return [1, -1, 2, -2]
    return list(range(1, cycle_size))


def passed_along(block, axis, distance):
    devices = range(lax.axis_size(axis))
    route = [((i - distance) % len(devices), i) for i in devices]
    return lax.ppermute(block, axis, route)


def gather_near(copies, short, long):
    boxes = copies
    if short:
        boxes = lax.all_to_all(copies, short, 0, 0, tiled=True)
    for axis in long:
        pieces = [boxes]
        for offset in cycle_offsets(lax.axis_size(axis)):
            pieces.append(passed_along(boxes, axis, offset))
        boxes = jnp.concatenate(pieces)
    return boxes


def local(positions, velocities, forces, charges, inverse_mass, occupancy, molecule):
    axes = ("gx", "gy", "gz")
    extents = [lax.axis_size(axis) for axis in axes]
    sizes = Sizes([float(extent) for extent in extents])
    short = tuple(axis for axis, extent in zip(axes, extents) if extent < 5)
    long = tuple(axis for axis, extent in zip(axes, extents) if extent >= 5)
    copies = math.prod([1] + [extent for extent in extents if extent < 5])
    count = copies * 5 ** len(long)

    vmem = pl.BlockSpec(memory_space=pltpu.VMEM)
    smem = pl.BlockSpec(memory_space=pltpu.SMEM)
    small = pltpu.CompilerParams(vmem_limit_bytes=8 * 1024 * 1024)
    block = jax.ShapeDtypeStruct((ROWS, LANES), jnp.float32)
    many = jax.ShapeDtypeStruct((copies, ROWS, LANES), jnp.float32)
    send, own, mid, mass, charge, label = pl.pallas_call(
        start_kernel,
        out_shape=(many, block, block, block, block, jax.ShapeDtypeStruct(molecule.shape, jnp.int32)),
        in_specs=[pl.BlockSpec(memory_space=pltpu.HBM)] * 6 + [smem],
        out_specs=(vmem,) * 6,
        scratch_shapes=[
            pltpu.VMEM(array.shape, array.dtype)
            for array in (positions, velocities, forces, charges, inverse_mass)
        ]
        + [pltpu.SemaphoreType.DMA((6,))],
        compiler_params=small,
        name="start",
    )(*[pltpu.with_memory_space_constraint(array, pltpu.HBM) for array in (positions, velocities, forces, charges, inverse_mass, molecule)], occupancy)

    pairs = 2 * LANES * LANES * 2 * count
    scratch = [
        pltpu.VMEM((ROWS * (count + 1), LANES), jnp.int32),
        pltpu.VMEM((count + 4, ROWS, LANES), jnp.int32),
        pltpu.VMEM((count + 4, ROWS, LANES), jnp.float32),
        pltpu.SMEM((count,), jnp.int32),
        pltpu.VMEM((3, 2 * LANES // ROWS, ROWS, LANES), jnp.int32),
        pltpu.VMEM((3, 2 * LANES, LANES), jnp.float32),
    ]
    cost = pl.CostEstimate(flops=26 * pairs, bytes_accessed=64 * pairs // LANES, transcendentals=pairs)

    boxes = gather_near(send, short, long).reshape(count * ROWS, LANES)
    send, own, mid = pl.pallas_call(
        functools.partial(middle_kernel, sizes),
        out_shape=(jax.ShapeDtypeStruct((6 * copies, LANES), jnp.float32), block, block),
        in_specs=[vmem] * 6,
        out_specs=(vmem,) * 3,
        scratch_shapes=scratch,
        compiler_params=small,
        cost_estimate=cost,
        name="middle",
    )(boxes, own, mid, mass, charge, label)
    places = gather_near(send.reshape(copies, 1, 6 * LANES), short, long)
    whole = jax.ShapeDtypeStruct(positions.shape, jnp.float32)
    return pl.pallas_call(
        functools.partial(last_kernel, sizes),
        out_shape=(whole, whole, whole),
        in_specs=[vmem] * 7,
        out_specs=(vmem,) * 3,
        scratch_shapes=scratch,
        compiler_params=small,
        cost_estimate=cost,
        name="last",
    )(boxes, places.reshape(6 * count, LANES), own, mid, mass, charge, label)


def solution(mesh):
    in_specs = (
        P(None, "gx", "gy", "gz", None),
        P(None, "gx", "gy", "gz", None),
        P(None, "gx", "gy", "gz", None),
        P("gx", "gy", "gz", None),
        P("gx", "gy", "gz", None),
        P("gx", "gy", "gz"),
        P("gx", "gy", "gz", None),
    )
    out_specs = (
        P(None, "gx", "gy", "gz", None),
        P(None, "gx", "gy", "gz", None),
        P(None, "gx", "gy", "gz", None),
    )
    return jax.shard_map(local, mesh=mesh, in_specs=in_specs, out_specs=out_specs, check_vma=False)
```

```python
import functools
import math

import jax
import jax.numpy as jnp
from jax import lax
from jax.experimental import pallas as pl
from jax.experimental.pallas import tpu as pltpu
from jax.sharding import PartitionSpec as P

cutoff_square = 4.0
soften_square = 0.25
time_step = 0.1
half_step = 0.05

LANES = 128
ROWS = 8
TIES = (128, 191)
FULL = 4294967296.0


class Sizes:
    def __init__(self, lengths):
        self.lengths = lengths
        self.unit = max(set(lengths), key=lengths.count)
        step = self.unit / FULL
        self.top = cutoff_square / step**2
        self.soft = soften_square / step**2
        self.ratio = [(length / self.unit) ** 2 for length in lengths]
        self.scale = [
            (1.0 / (cutoff_square * cutoff_square)) * step * (length / FULL) for length in lengths
        ]
        self.seam = [length * length / 4 < cutoff_square for length in lengths]


def row_constant(values):
    row = lax.broadcasted_iota(jnp.int32, (ROWS, LANES), 0) // 2
    out = jnp.zeros((ROWS, LANES), jnp.float32)
    for c, value in enumerate(values):
        out = jnp.where(row == c, jnp.float32(value), out)
    return out


def to_steps(values, inverse):
    turns = values * inverse
    turns = turns - jnp.round(turns)
    turns = jnp.where(turns >= 0.5, -0.5, turns)
    return (turns * jnp.float32(FULL)).astype(jnp.int32)


def seam_shift(places, sizes):
    row = lax.broadcasted_iota(jnp.int32, (ROWS, LANES), 0) // 2
    shift = jnp.zeros((ROWS, LANES), jnp.int32)
    for c, length in enumerate(sizes.lengths):
        if sizes.seam[c]:
            near = jnp.where(jnp.abs(places) < length / 4, TIES[0], TIES[1])
            shift = jnp.where(row == c, near, shift)
    return shift


def pair_weight(target, source, charge, sizes):
    parts = [(t - s).astype(jnp.float32) for t, s in zip(target, source)]
    squared = None
    for part, ratio in sorted(zip(parts, sizes.ratio), key=lambda item: item[1] != 1.0):
        square = part * part
        if ratio != 1.0:
            square = square * jnp.float32(ratio)
        squared = square if squared is None else squared + square
    switch = jnp.maximum(jnp.float32(sizes.top) - squared, 0.0)
    root = lax.rsqrt(squared + jnp.float32(sizes.soft))
    first = switch * root
    return parts, (first * root) * (first * charge)


def start_kernel(pos, vel, frc, chg, imass, lab, occ, send, own, mid, mass, charge, label,
                 pos_in, vel_in, frc_in, chg_in, imass_in, sems):
    copies = [
        pltpu.make_async_copy(source, target, sems.at[i])
        for i, (source, target) in enumerate(
            ((pos, pos_in), (vel, vel_in), (frc, frc_in), (chg, chg_in), (imass, imass_in), (lab, label))
        )
    ]
    for copy in copies:
        copy.start()
    for copy in copies:
        copy.wait()
    live = lax.broadcasted_iota(jnp.int32, (1, 2 * LANES), 1) < occ[0, 0, 0]
    live_charge = jnp.where(live, chg_in[0, 0], 0.0)
    inverse = imass_in[0, 0]
    for h in range(2):
        cut = slice(h * LANES, (h + 1) * LANES)
        for c in range(3):
            r = slice(2 * c + h, 2 * c + h + 1)
            midway = vel_in[c, 0, 0] + half_step * inverse * frc_in[c, 0, 0]
            places = pos_in[c, 0, 0] + time_step * midway
            own[r, :] = places[:, cut]
            mid[r, :] = midway[:, cut]
            mass[r, :] = inverse[:, cut]
            charge[r, :] = live_charge[:, cut]
        r = slice(6 + h, 7 + h)
        own[r, :] = live_charge[:, cut]
        mid[r, :] = jnp.zeros((1, LANES), jnp.float32)
        mass[r, :] = jnp.zeros((1, LANES), jnp.float32)
        charge[r, :] = jnp.zeros((1, LANES), jnp.float32)
    block = own[...]
    for b in range(send.shape[0]):
        send[b] = block


def prepare(own, charge, labels, sizes):
    mine = to_steps(own[...], row_constant([1.0 / length for length in sizes.lengths]))
    aim = mine + seam_shift(own[...], sizes)
    columns = jnp.transpose(aim)

    def spread(array):
        line = jnp.concatenate([array[0:1, :], array[1:2, :]], axis=1)
        return jnp.broadcast_to(line, (ROWS, 2 * LANES))

    def shifted(array):
        return pltpu.roll(pltpu.roll(array, 2 * LANES - 3, 1), 0, 1, stride=1, stride_axis=0)

    here = [spread(aim[2 * c : 2 * c + 2]) for c in range(3)]
    there = [shifted(spread(mine[2 * c : 2 * c + 2])) for c in range(3)]
    charge_there = shifted(spread(charge[0:2, :]))
    label = jnp.broadcast_to(labels[0, 0], (ROWS, 2 * LANES))
    slot = lax.broadcasted_iota(jnp.int32, (ROWS, 2 * LANES), 1)
    away = lax.broadcasted_iota(jnp.int32, (ROWS, 2 * LANES), 0)
    other = slot + 3 - away
    same = (shifted(label) == label) & (other >= 0) & (other < 2 * LANES) & (away < 7)
    parts, base = pair_weight(here, there, jnp.where(same, charge_there, 0.0), sizes)
    return columns, [jnp.sum(base * parts[c], axis=0, keepdims=True) for c in range(3)]


def add_tiles(tiles, columns, targets, sums, sizes):
    for g in range(2 * LANES // ROWS):
        if columns is None:
            target = [targets[c, g] for c in range(3)]
        else:
            half, spot = divmod(g * ROWS, LANES)
            target = [
                jnp.broadcast_to(
                    columns[spot : spot + ROWS, 2 * c + half : 2 * c + half + 1], (ROWS, LANES)
                )
                for c in range(3)
            ]
            for c in range(3):
                targets[c, g] = target[c]
        added = [None] * 3
        for source, charge in tiles:
            parts, base = pair_weight(target, source, charge, sizes)
            for c in range(3):
                product = base * parts[c]
                if added[c] is None and columns is None:
                    added[c] = sums[c, ROWS * g : ROWS * g + ROWS, :]
                added[c] = product if added[c] is None else added[c] + product
        for c in range(3):
            rows = slice(ROWS * g, ROWS * g + ROWS)
            sums[c, rows, :] = added[c]


def force_of(charges, places, per, own, charge, labels, steps, packed, packed_charges, offsets,
             targets, sums, sizes):
    count = charges.shape[0] // ROWS
    stride = 2 if count % 2 == 0 else 1
    lane = lax.broadcasted_iota(jnp.int32, (ROWS, LANES), 1)
    columns, within = prepare(own, charge, labels, sizes)

    inverses = {}
    for k in range(pl.cdiv(places.shape[0], ROWS)):
        begin = (ROWS * k) % per
        if begin not in inverses:
            axis = lax.rem(lax.broadcasted_iota(jnp.int32, (ROWS, LANES), 0) + begin, per) // 2
            inverse = jnp.zeros((ROWS, LANES), jnp.float32)
            for c, length in enumerate(sizes.lengths):
                inverse = jnp.where(axis == c, jnp.float32(1.0 / length), inverse)
            inverses[begin] = inverse
        size = min(ROWS, places.shape[0] - ROWS * k)
        rows = slice(ROWS * k, ROWS * k + size)
        steps[rows, :] = to_steps(places[rows, :], inverses[begin][:size])

    def one(ref, row):
        return jnp.broadcast_to(ref[pl.ds(row, 1), :], (ROWS, LANES))

    def heads(k, unused, fresh=None):
        boxes = [k * stride + u for u in range(stride)]
        tiles = [
            ([one(steps, b * per + 2 * c) for c in range(3)], one(charges, b * ROWS + 6))
            for b in boxes
        ]
        add_tiles(tiles, fresh, targets, sums, sizes)
        for b in boxes:
            position = offsets[b]
            tile = position // LANES
            begin = lax.rem(position, LANES)
            late = lane >= begin
            moved = pltpu.roll(steps[pl.ds(b * per, ROWS), :], begin, 1)
            pltpu.store(packed.at[tile], moved, mask=late)
            packed[tile + 1] = moved
            box = charges[pl.ds(pl.multiple_of(b * ROWS, ROWS), ROWS), :]
            moved = pltpu.roll(box, begin, 1)
            pltpu.store(packed_charges.at[tile], moved, mask=late)
            packed_charges[tile + 1] = jnp.where(late, 0.0, moved)
        return unused

    live = jnp.where(
        charges[pl.ds(7, count, stride=ROWS), :] != 0.0, lane[:1].astype(jnp.float32) + 1.0, 0.0
    )
    filled = jnp.max(live, axis=1, keepdims=True).astype(jnp.int32)
    position = jnp.int32(0)
    for b in range(count):
        offsets[b] = position
        position = position + filled[b, 0]
    heads(0, 0, columns)
    lax.fori_loop(1, count // stride, heads, 0)
    filled_tiles = (position + (LANES - 1)) // LANES
    for u in range(stride):
        packed_charges[filled_tiles + u] = jnp.zeros((ROWS, LANES), jnp.float32)

    def tails(k, unused):
        tiles = [
            (
                [
                    jnp.broadcast_to(packed[t, 2 * c + 1 : 2 * c + 2, :], (ROWS, LANES))
                    for c in range(3)
                ],
                jnp.broadcast_to(packed_charges[t, 7:8, :], (ROWS, LANES)),
            )
            for t in [k * stride + u for u in range(stride)]
        ]
        add_tiles(tiles, None, targets, sums, sizes)
        return unused

    lax.fori_loop(0, (filled_tiles + stride - 1) // stride, tails, 0)

    row = lax.broadcasted_iota(jnp.int32, (ROWS, LANES), 0)
    ones = jnp.ones((ROWS, LANES), jnp.bfloat16)
    result = jnp.zeros((ROWS, LANES), jnp.float32)
    for c in range(3):
        left = sums[c]
        total = jnp.zeros((ROWS, 2 * LANES), jnp.float32)
        for piece in range(3):
            part = left.astype(jnp.bfloat16)
            left = left - part.astype(jnp.float32)
            total = total + lax.dot_general(
                ones, part, (((1,), (1,)), ((), ())), preferred_element_type=jnp.float32
            )
        total = (total - within[c]) * jnp.float32(sizes.scale[c])
        for h in range(2):
            result = jnp.where(row == 2 * c + h, total[:, h * LANES : (h + 1) * LANES], result)
    return charge[...] * result


def middle_kernel(sizes, boxes, own, mid, mass, charge, labels, send, own_out, mid_out, *scratch):
    force = force_of(boxes, boxes, ROWS, own, charge, labels, *scratch, sizes)
    kick = half_step * mass[...] * force
    midway = (mid[...] + kick) + kick
    places = own[...] + time_step * midway
    row = lax.broadcasted_iota(jnp.int32, (ROWS, LANES), 0)
    block = jnp.where(row < 6, places, own[...])
    own_out[...] = block
    mid_out[...] = midway
    rows = send.shape[0]
    for k in range(pl.cdiv(rows, ROWS)):
        begin = (ROWS * k) % 6
        early = block if begin == 0 else pltpu.roll(block, ROWS - begin, 0)
        late = pltpu.roll(block, (6 - begin) % ROWS, 0)
        twice = jnp.where(row < 6 - begin, early, late)
        size = min(ROWS, rows - ROWS * k)
        send[ROWS * k : ROWS * k + size, :] = twice[:size]


def last_kernel(sizes, boxes, places_in, own, mid, mass, charge, labels, pos, vel, frc, *scratch):
    force = force_of(boxes, places_in, 6, own, charge, labels, *scratch, sizes)
    velocity = mid[...] + half_step * mass[...] * force
    places = own[...]
    for c in range(3):
        for h in range(2):
            r = slice(2 * c + h, 2 * c + h + 1)
            cut = slice(h * LANES, (h + 1) * LANES)
            pos[c, 0, 0, :, cut] = places[r, :]
            vel[c, 0, 0, :, cut] = velocity[r, :]
            frc[c, 0, 0, :, cut] = force[r, :]


def cycle_offsets(cycle_size):
    if cycle_size >= 5:
        return [1, -1, 2, -2]
    return list(range(1, cycle_size))


def passed_along(block, axis, distance):
    devices = range(lax.axis_size(axis))
    route = [((i - distance) % len(devices), i) for i in devices]
    return lax.ppermute(block, axis, route)


def gather_near(copies, short, long):
    boxes = copies
    if short:
        boxes = lax.all_to_all(copies, short, 0, 0, tiled=True)
    for axis in long:
        pieces = [boxes]
        for offset in cycle_offsets(lax.axis_size(axis)):
            pieces.append(passed_along(boxes, axis, offset))
        boxes = jnp.concatenate(pieces)
    return boxes


def local(positions, velocities, forces, charges, inverse_mass, occupancy, molecule):
    axes = ("gx", "gy", "gz")
    extents = [lax.axis_size(axis) for axis in axes]
    sizes = Sizes([float(extent) for extent in extents])
    short = tuple(axis for axis, extent in zip(axes, extents) if extent < 5)
    long = tuple(axis for axis, extent in zip(axes, extents) if extent >= 5)
    copies = math.prod([1] + [extent for extent in extents if extent < 5])
    count = copies * 5 ** len(long)

    vmem = pl.BlockSpec(memory_space=pltpu.VMEM)
    smem = pl.BlockSpec(memory_space=pltpu.SMEM)
    small = pltpu.CompilerParams(vmem_limit_bytes=8 * 1024 * 1024)
    block = jax.ShapeDtypeStruct((ROWS, LANES), jnp.float32)
    many = jax.ShapeDtypeStruct((copies, ROWS, LANES), jnp.float32)
    send, own, mid, mass, charge, label = pl.pallas_call(
        start_kernel,
        out_shape=(many, block, block, block, block, jax.ShapeDtypeStruct(molecule.shape, jnp.int32)),
        in_specs=[pl.BlockSpec(memory_space=pltpu.HBM)] * 6 + [smem],
        out_specs=(vmem,) * 6,
        scratch_shapes=[
            pltpu.VMEM(array.shape, array.dtype)
            for array in (positions, velocities, forces, charges, inverse_mass)
        ]
        + [pltpu.SemaphoreType.DMA((6,))],
        compiler_params=small,
        name="start",
    )(*[pltpu.with_memory_space_constraint(array, pltpu.HBM) for array in (positions, velocities, forces, charges, inverse_mass, molecule)], occupancy)

    pairs = 2 * LANES * LANES * 2 * count
    scratch = [
        pltpu.VMEM((ROWS * (count + 1), LANES), jnp.int32),
        pltpu.VMEM((count + 4, ROWS, LANES), jnp.int32),
        pltpu.VMEM((count + 4, ROWS, LANES), jnp.float32),
        pltpu.SMEM((count,), jnp.int32),
        pltpu.VMEM((3, 2 * LANES // ROWS, ROWS, LANES), jnp.int32),
        pltpu.VMEM((3, 2 * LANES, LANES), jnp.float32),
    ]
    cost = pl.CostEstimate(flops=26 * pairs, bytes_accessed=64 * pairs // LANES, transcendentals=pairs)

    boxes = gather_near(send, short, long).reshape(count * ROWS, LANES)
    send, own, mid = pl.pallas_call(
        functools.partial(middle_kernel, sizes),
        out_shape=(jax.ShapeDtypeStruct((6 * copies, LANES), jnp.float32), block, block),
        in_specs=[vmem] * 6,
        out_specs=(vmem,) * 3,
        scratch_shapes=scratch,
        compiler_params=small,
        cost_estimate=cost,
        name="middle",
    )(boxes, own, mid, mass, charge, label)
    places = gather_near(send.reshape(copies, 1, 6 * LANES), short, long)
    whole = jax.ShapeDtypeStruct(positions.shape, jnp.float32)
    return pl.pallas_call(
        functools.partial(last_kernel, sizes),
        out_shape=(whole, whole, whole),
        in_specs=[vmem] * 7,
        out_specs=(vmem,) * 3,
        scratch_shapes=scratch,
        compiler_params=small,
        cost_estimate=cost,
        name="last",
    )(boxes, places.reshape(6 * count, LANES), own, mid, mass, charge, label)


def solution(mesh):
    in_specs = (
        P(None, "gx", "gy", "gz", None),
        P(None, "gx", "gy", "gz", None),
        P(None, "gx", "gy", "gz", None),
        P("gx", "gy", "gz", None),
        P("gx", "gy", "gz", None),
        P("gx", "gy", "gz"),
        P("gx", "gy", "gz", None),
    )
    out_specs = (
        P(None, "gx", "gy", "gz", None),
        P(None, "gx", "gy", "gz", None),
        P(None, "gx", "gy", "gz", None),
    )
    return jax.shard_map(local, mesh=mesh, in_specs=in_specs, out_specs=out_specs, check_vma=False)
```

```python
import functools
import math

import jax
import jax.numpy as jnp
from jax import lax
from jax.experimental import pallas as pl
from jax.experimental.pallas import tpu as pltpu
from jax.sharding import PartitionSpec as P

cutoff_square = 4.0
soften_square = 0.25
time_step = 0.1
half_step = 0.05

ROWS = 8
TIES = (128, 191)
FULL = 4294967296.0


class Sizes:
    def __init__(self, lengths, slots):
        self.half = slots // 2
        self.lengths = lengths
        self.unit = max(set(lengths), key=lengths.count)
        step = self.unit / FULL
        self.top = cutoff_square / step**2
        self.soft = soften_square / step**2
        self.ratio = [(length / self.unit) ** 2 for length in lengths]
        self.scale = [
            (1.0 / (cutoff_square * cutoff_square)) * step * (length / FULL) for length in lengths
        ]
        self.seam = [length * length / 4 < cutoff_square for length in lengths]


def row_constant(values, half):
    row = lax.broadcasted_iota(jnp.int32, (ROWS, half), 0) // 2
    out = jnp.zeros((ROWS, half), jnp.float32)
    for c, value in enumerate(values):
        out = jnp.where(row == c, jnp.float32(value), out)
    return out


def to_steps(values, inverse):
    turns = values * inverse
    turns = turns - jnp.round(turns)
    turns = jnp.where(turns >= 0.5, -0.5, turns)
    return (turns * jnp.float32(FULL)).astype(jnp.int32)


def seam_shift(places, sizes):
    row = lax.broadcasted_iota(jnp.int32, (ROWS, sizes.half), 0) // 2
    shift = jnp.zeros((ROWS, sizes.half), jnp.int32)
    for c, length in enumerate(sizes.lengths):
        if sizes.seam[c]:
            near = jnp.where(jnp.abs(places) < length / 4, TIES[0], TIES[1])
            shift = jnp.where(row == c, near, shift)
    return shift


def pair_weight(target, source, charge, sizes):
    parts = [(t - s).astype(jnp.float32) for t, s in zip(target, source)]
    squared = None
    for part, ratio in sorted(zip(parts, sizes.ratio), key=lambda item: item[1] != 1.0):
        square = part * part
        if ratio != 1.0:
            square = square * jnp.float32(ratio)
        squared = square if squared is None else squared + square
    switch = jnp.maximum(jnp.float32(sizes.top) - squared, 0.0)
    root = lax.rsqrt(squared + jnp.float32(sizes.soft))
    first = switch * root
    return parts, (first * root) * (first * charge)


def start_kernel(sizes, pos, vel, frc, chg, imass, lab, occ, send, own, mid, mass, charge, label,
                 pos_in, vel_in, frc_in, chg_in, imass_in, sems):
    copies = [
        pltpu.make_async_copy(source, target, sems.at[i])
        for i, (source, target) in enumerate(
            ((pos, pos_in), (vel, vel_in), (frc, frc_in), (chg, chg_in), (imass, imass_in), (lab, label))
        )
    ]
    for copy in copies:
        copy.start()
    for copy in copies:
        copy.wait()
    live = lax.broadcasted_iota(jnp.int32, (1, 2 * sizes.half), 1) < occ[0, 0, 0]
    live_charge = jnp.where(live, chg_in[0, 0], 0.0)
    inverse = imass_in[0, 0]
    for h in range(2):
        cut = slice(h * sizes.half, (h + 1) * sizes.half)
        for c in range(3):
            r = slice(2 * c + h, 2 * c + h + 1)
            midway = vel_in[c, 0, 0] + half_step * inverse * frc_in[c, 0, 0]
            places = pos_in[c, 0, 0] + time_step * midway
            own[r, :] = places[:, cut]
            mid[r, :] = midway[:, cut]
            mass[r, :] = inverse[:, cut]
            charge[r, :] = live_charge[:, cut]
        r = slice(6 + h, 7 + h)
        own[r, :] = live_charge[:, cut]
        mid[r, :] = jnp.zeros((1, sizes.half), jnp.float32)
        mass[r, :] = jnp.zeros((1, sizes.half), jnp.float32)
        charge[r, :] = jnp.zeros((1, sizes.half), jnp.float32)
    block = own[...]
    for b in range(send.shape[0]):
        send[b] = block


def prepare(own, charge, labels, sizes):
    mine = to_steps(own[...], row_constant([1.0 / length for length in sizes.lengths], sizes.half))
    aim = mine + seam_shift(own[...], sizes)
    columns = jnp.transpose(aim)

    def spread(array):
        line = jnp.concatenate([array[0:1, :], array[1:2, :]], axis=1)
        return jnp.broadcast_to(line, (ROWS, 2 * sizes.half))

    def shifted(array):
        return pltpu.roll(pltpu.roll(array, 2 * sizes.half - 3, 1), 0, 1, stride=1, stride_axis=0)

    here = [spread(aim[2 * c : 2 * c + 2]) for c in range(3)]
    there = [shifted(spread(mine[2 * c : 2 * c + 2])) for c in range(3)]
    charge_there = shifted(spread(charge[0:2, :]))
    label = jnp.broadcast_to(labels[0, 0], (ROWS, 2 * sizes.half))
    slot = lax.broadcasted_iota(jnp.int32, (ROWS, 2 * sizes.half), 1)
    away = lax.broadcasted_iota(jnp.int32, (ROWS, 2 * sizes.half), 0)
    other = slot + 3 - away
    same = (shifted(label) == label) & (other >= 0) & (other < 2 * sizes.half) & (away < 7)
    parts, base = pair_weight(here, there, jnp.where(same, charge_there, 0.0), sizes)
    return columns, [jnp.sum(base * parts[c], axis=0, keepdims=True) for c in range(3)]


def add_tiles(tiles, columns, targets, sums, sizes):
    for g in range(2 * sizes.half // ROWS):
        if columns is None:
            target = [targets[c, g] for c in range(3)]
        else:
            half, spot = divmod(g * ROWS, sizes.half)
            target = [
                jnp.broadcast_to(
                    columns[spot : spot + ROWS, 2 * c + half : 2 * c + half + 1], (ROWS, sizes.half)
                )
                for c in range(3)
            ]
            for c in range(3):
                targets[c, g] = target[c]
        added = [None] * 3
        for source, charge in tiles:
            parts, base = pair_weight(target, source, charge, sizes)
            for c in range(3):
                product = base * parts[c]
                if added[c] is None and columns is None:
                    added[c] = sums[c, ROWS * g : ROWS * g + ROWS, :]
                added[c] = product if added[c] is None else added[c] + product
        for c in range(3):
            rows = slice(ROWS * g, ROWS * g + ROWS)
            sums[c, rows, :] = added[c]


def force_of(charges, places, per, own, charge, labels, steps, packed, packed_charges, offsets,
             targets, sums, sizes):
    count = charges.shape[0] // ROWS
    stride = 2 if count % 2 == 0 else 1
    lane = lax.broadcasted_iota(jnp.int32, (ROWS, sizes.half), 1)
    columns, within = prepare(own, charge, labels, sizes)

    inverses = {}
    for k in range(pl.cdiv(places.shape[0], ROWS)):
        begin = (ROWS * k) % per
        if begin not in inverses:
            axis = lax.rem(lax.broadcasted_iota(jnp.int32, (ROWS, sizes.half), 0) + begin, per) // 2
            inverse = jnp.zeros((ROWS, sizes.half), jnp.float32)
            for c, length in enumerate(sizes.lengths):
                inverse = jnp.where(axis == c, jnp.float32(1.0 / length), inverse)
            inverses[begin] = inverse
        size = min(ROWS, places.shape[0] - ROWS * k)
        rows = slice(ROWS * k, ROWS * k + size)
        steps[rows, :] = to_steps(places[rows, :], inverses[begin][:size])

    def one(ref, row):
        return jnp.broadcast_to(ref[pl.ds(row, 1), :], (ROWS, sizes.half))

    def heads(k, unused, fresh=None):
        boxes = [k * stride + u for u in range(stride)]
        tiles = [
            ([one(steps, b * per + 2 * c) for c in range(3)], one(charges, b * ROWS + 6))
            for b in boxes
        ]
        add_tiles(tiles, fresh, targets, sums, sizes)
        for b in boxes:
            position = offsets[b]
            tile = position // sizes.half
            begin = lax.rem(position, sizes.half)
            late = lane >= begin
            moved = pltpu.roll(steps[pl.ds(b * per, ROWS), :], begin, 1)
            pltpu.store(packed.at[tile], moved, mask=late)
            packed[tile + 1] = moved
            box = charges[pl.ds(pl.multiple_of(b * ROWS, ROWS), ROWS), :]
            moved = pltpu.roll(box, begin, 1)
            pltpu.store(packed_charges.at[tile], moved, mask=late)
            packed_charges[tile + 1] = jnp.where(late, 0.0, moved)
        return unused

    live = jnp.where(
        charges[pl.ds(7, count, stride=ROWS), :] != 0.0, lane[:1].astype(jnp.float32) + 1.0, 0.0
    )
    filled = jnp.max(live, axis=1, keepdims=True).astype(jnp.int32)
    position = jnp.int32(0)
    for b in range(count):
        offsets[b] = position
        position = position + filled[b, 0]
    heads(0, 0, columns)
    lax.fori_loop(1, count // stride, heads, 0)
    filled_tiles = (position + (sizes.half - 1)) // sizes.half
    for u in range(stride):
        packed_charges[filled_tiles + u] = jnp.zeros((ROWS, sizes.half), jnp.float32)

    def tails(k, unused):
        tiles = [
            (
                [
                    jnp.broadcast_to(packed[t, 2 * c + 1 : 2 * c + 2, :], (ROWS, sizes.half))
                    for c in range(3)
                ],
                jnp.broadcast_to(packed_charges[t, 7:8, :], (ROWS, sizes.half)),
            )
            for t in [k * stride + u for u in range(stride)]
        ]
        add_tiles(tiles, None, targets, sums, sizes)
        return unused

    lax.fori_loop(0, (filled_tiles + stride - 1) // stride, tails, 0)

    row = lax.broadcasted_iota(jnp.int32, (ROWS, sizes.half), 0)
    ones = jnp.ones((ROWS, sizes.half), jnp.bfloat16)
    result = jnp.zeros((ROWS, sizes.half), jnp.float32)
    for c in range(3):
        left = sums[c]
        total = jnp.zeros((ROWS, 2 * sizes.half), jnp.float32)
        for piece in range(3):
            part = left.astype(jnp.bfloat16)
            left = left - part.astype(jnp.float32)
            total = total + lax.dot_general(
                ones, part, (((1,), (1,)), ((), ())), preferred_element_type=jnp.float32
            )
        total = (total - within[c]) * jnp.float32(sizes.scale[c])
        for h in range(2):
            result = jnp.where(row == 2 * c + h, total[:, h * sizes.half : (h + 1) * sizes.half], result)
    return charge[...] * result


def middle_kernel(sizes, boxes, own, mid, mass, charge, labels, send, own_out, mid_out, *scratch):
    force = force_of(boxes, boxes, ROWS, own, charge, labels, *scratch, sizes)
    kick = half_step * mass[...] * force
    midway = (mid[...] + kick) + kick
    places = own[...] + time_step * midway
    row = lax.broadcasted_iota(jnp.int32, (ROWS, sizes.half), 0)
    block = jnp.where(row < 6, places, own[...])
    own_out[...] = block
    mid_out[...] = midway
    rows = send.shape[0]
    for k in range(pl.cdiv(rows, ROWS)):
        begin = (ROWS * k) % 6
        early = block if begin == 0 else pltpu.roll(block, ROWS - begin, 0)
        late = pltpu.roll(block, (6 - begin) % ROWS, 0)
        twice = jnp.where(row < 6 - begin, early, late)
        size = min(ROWS, rows - ROWS * k)
        send[ROWS * k : ROWS * k + size, :] = twice[:size]


def last_kernel(sizes, boxes, places_in, own, mid, mass, charge, labels, pos, vel, frc, *scratch):
    force = force_of(boxes, places_in, 6, own, charge, labels, *scratch, sizes)
    velocity = mid[...] + half_step * mass[...] * force
    places = own[...]
    for c in range(3):
        for h in range(2):
            r = slice(2 * c + h, 2 * c + h + 1)
            cut = slice(h * sizes.half, (h + 1) * sizes.half)
            pos[c, 0, 0, :, cut] = places[r, :]
            vel[c, 0, 0, :, cut] = velocity[r, :]
            frc[c, 0, 0, :, cut] = force[r, :]


def cycle_offsets(cycle_size):
    if cycle_size >= 5:
        return [1, -1, 2, -2]
    return list(range(1, cycle_size))


def passed_along(block, axis, distance):
    devices = range(lax.axis_size(axis))
    route = [((i - distance) % len(devices), i) for i in devices]
    return lax.ppermute(block, axis, route)


def gather_near(copies, short, long):
    boxes = copies
    if short:
        boxes = lax.all_to_all(copies, short, 0, 0, tiled=True)
    for axis in long:
        pieces = [boxes]
        for offset in cycle_offsets(lax.axis_size(axis)):
            pieces.append(passed_along(boxes, axis, offset))
        boxes = jnp.concatenate(pieces)
    return boxes


def local(positions, velocities, forces, charges, inverse_mass, occupancy, molecule):
    axes = ("gx", "gy", "gz")
    extents = [lax.axis_size(axis) for axis in axes]
    sizes = Sizes([float(extent) for extent in extents], positions.shape[-1])
    short = tuple(axis for axis, extent in zip(axes, extents) if extent < 5)
    long = tuple(axis for axis, extent in zip(axes, extents) if extent >= 5)
    copies = math.prod([1] + [extent for extent in extents if extent < 5])
    count = copies * 5 ** len(long)

    vmem = pl.BlockSpec(memory_space=pltpu.VMEM)
    smem = pl.BlockSpec(memory_space=pltpu.SMEM)
    small = pltpu.CompilerParams(vmem_limit_bytes=8 * 1024 * 1024)
    block = jax.ShapeDtypeStruct((ROWS, sizes.half), jnp.float32)
    many = jax.ShapeDtypeStruct((copies, ROWS, sizes.half), jnp.float32)
    send, own, mid, mass, charge, label = pl.pallas_call(
        functools.partial(start_kernel, sizes),
        out_shape=(many, block, block, block, block, jax.ShapeDtypeStruct(molecule.shape, jnp.int32)),
        in_specs=[pl.BlockSpec(memory_space=pltpu.HBM)] * 6 + [smem],
        out_specs=(vmem,) * 6,
        scratch_shapes=[
            pltpu.VMEM(array.shape, array.dtype)
            for array in (positions, velocities, forces, charges, inverse_mass)
        ]
        + [pltpu.SemaphoreType.DMA((6,))],
        compiler_params=small,
        name="start",
    )(*[pltpu.with_memory_space_constraint(array, pltpu.HBM) for array in (positions, velocities, forces, charges, inverse_mass, molecule)], occupancy)

    pairs = 2 * sizes.half * sizes.half * 2 * count
    scratch = [
        pltpu.VMEM((ROWS * (count + 1), sizes.half), jnp.int32),
        pltpu.VMEM((count + 4, ROWS, sizes.half), jnp.int32),
        pltpu.VMEM((count + 4, ROWS, sizes.half), jnp.float32),
        pltpu.SMEM((count,), jnp.int32),
        pltpu.VMEM((3, 2 * sizes.half // ROWS, ROWS, sizes.half), jnp.int32),
        pltpu.VMEM((3, 2 * sizes.half, sizes.half), jnp.float32),
    ]
    cost = pl.CostEstimate(flops=26 * pairs, bytes_accessed=64 * pairs // sizes.half, transcendentals=pairs)

    boxes = gather_near(send, short, long).reshape(count * ROWS, sizes.half)
    send, own, mid = pl.pallas_call(
        functools.partial(middle_kernel, sizes),
        out_shape=(jax.ShapeDtypeStruct((6 * copies, sizes.half), jnp.float32), block, block),
        in_specs=[vmem] * 6,
        out_specs=(vmem,) * 3,
        scratch_shapes=scratch,
        compiler_params=small,
        cost_estimate=cost,
        name="middle",
    )(boxes, own, mid, mass, charge, label)
    places = gather_near(send.reshape(copies, 1, 6 * sizes.half), short, long)
    whole = jax.ShapeDtypeStruct(positions.shape, jnp.float32)
    return pl.pallas_call(
        functools.partial(last_kernel, sizes),
        out_shape=(whole, whole, whole),
        in_specs=[vmem] * 7,
        out_specs=(vmem,) * 3,
        scratch_shapes=scratch,
        compiler_params=small,
        cost_estimate=cost,
        name="last",
    )(boxes, places.reshape(6 * count, sizes.half), own, mid, mass, charge, label)


def solution(mesh):
    in_specs = (
        P(None, "gx", "gy", "gz", None),
        P(None, "gx", "gy", "gz", None),
        P(None, "gx", "gy", "gz", None),
        P("gx", "gy", "gz", None),
        P("gx", "gy", "gz", None),
        P("gx", "gy", "gz"),
        P("gx", "gy", "gz", None),
    )
    out_specs = (
        P(None, "gx", "gy", "gz", None),
        P(None, "gx", "gy", "gz", None),
        P(None, "gx", "gy", "gz", None),
    )
    return jax.shard_map(local, mesh=mesh, in_specs=in_specs, out_specs=out_specs, check_vma=False)
```
